16 devices in a mesh: dp: 16 (over z, y, x, core).
Axes of the slice: x: 2, y: 2, z: 2, core: 2. Of those that a mesh axis runs over, the one named last changes fastest.
Arguments:
- grad_local: float32 [16, 2500608], P('dp')
- params: float32 [2500608], P('dp')
- accumulator: float32 [2500608], P('dp')
- learn_rate: float32 [], replicated
- clip_max: float32 [], replicated
Outputs:
- output 1: float32 [2500608], P('dp')
- output 2: float32 [2500608], P('dp')
- output 3: bfloat16 [2500608], replicated
- output 4: float32 [], replicated
All inputs are finite; a program needn't handle non-finite values.
Results may differ from the reference program's by a relative error of at most 0.001.
Values sent between devices are 32-bit elements.
A program may use at most 1 GiB of HBM per device.

```python
import math
import jax
import jax.numpy as jnp

DEVICES = 16
N_PARAMS = 2500608
EPS = 1e-10


def setup_inputs(seed: int = 0) -> dict:
    root_key = jax.random.key(seed)
    k_grad, k_par, k_acc, k_rate, k_clip = jax.random.split(root_key, 5)
    grad_local = jax.random.normal(k_grad, (DEVICES, N_PARAMS), jnp.float32) * math.sqrt(DEVICES)
    params = jax.random.normal(k_par, (N_PARAMS,), jnp.float32) * 0.1
    accumulator = jax.random.uniform(k_acc, (N_PARAMS,), jnp.float32, 0.05, 0.4)
    learn_rate = jnp.exp(jax.random.uniform(k_rate, (), jnp.float32, math.log(0.03), math.log(0.5)))
    clip_frac = jax.random.uniform(k_clip, (), jnp.float32, 0.3, 0.6)
    clip_max = clip_frac * math.sqrt(N_PARAMS)
    return {"grad_local": grad_local, "params": params, "accumulator": accumulator, "learn_rate": learn_rate, "clip_max": clip_max}


def reference(grad_local, params, accumulator, learn_rate, clip_max):
    mean_grad = jnp.sum(grad_local, axis=0) / DEVICES
    grad_norm = jnp.sqrt(jnp.sum(mean_grad * mean_grad))
    clip_scale = jnp.minimum(1.0, clip_max / grad_norm)
    clipped = mean_grad * clip_scale
    accum_new = accumulator + clipped * clipped
    param_new = params - learn_rate * clipped / (jnp.sqrt(accum_new) + EPS)
    return (param_new, accum_new, param_new.astype(jnp.bfloat16), grad_norm)
```

```python
import functools
import jax
import jax.numpy as jnp
from jax import lax
from jax.sharding import PartitionSpec as P
from jax.experimental import pallas as pl
from jax.experimental.pallas import tpu as pltpu

EPS = 1e-10
LANES = 128
X, Y, Z = 1, 2, 4
ORDERS = ((X, Y, Z), (Y, Z, X), (Z, X, Y))
MESH = pl.DeviceIdType.MESH


def kernel(
    blk, thr, groups,
    rate_ref, clip_ref, grad_hbm, par_hbm, acc_hbm,
    newp_ref, newa_ref, copy_ref, norm_ref,
    own, part, recv, full, par, acc, slots,
    load_sem, pa_sem, d2d_send, d2d_recv, rs_send, rs_recv,
    nrm_send, nrm_recv, ag_send, ag_recv, fwd_send, fwd_recv,
):
    me = lax.axis_index("dp")
    core = me % 2
    chip = me // 2
    x, y, z = chip % 2, (chip // 2) % 2, chip // 4
    partner = me + 1 - 2 * core
    across = {X: me + 2 - 4 * x, Y: me + 4 - 8 * y, Z: me + 8 - 16 * z}

    def base(m, c):
        xc = 1 - x if m & X else x
        yc = 1 - y if m & Y else y
        zc = 1 - z if m & Z else z
        return blk * (2 * (4 * zc + 2 * yc + xc) + c)

    def rows(m, t, c):
        return pl.ds(base(m, c) + thr * t, thr)

    unit = pl.ds(0, thr)

    def remote(src, dst, send, rcv, dev):
        return pltpu.make_async_remote_copy(
            src_ref=src, dst_ref=dst, send_sem=send, recv_sem=rcv,
            device_id=(dev,), device_id_type=MESH)

    order = []
    for pick in (
        lambda a, b, c: a + b + c, lambda a, b, c: a + b, lambda a, b, c: a + c, lambda a, b, c: a,
        lambda a, b, c: b + c, lambda a, b, c: b, lambda a, b, c: c, lambda a, b, c: 0,
    ):
        for t, dims in enumerate(ORDERS):
            order.append((pick(*dims), t))

    loads = {}
    for m, t in order:
        cp = pltpu.make_async_copy(
            grad_hbm.at[rows(m, t, core)], own.at[m, t, unit], load_sem.at[m, t])
        cp.start()
        loads[m, t] = cp
    par_cp = pltpu.make_async_copy(par_hbm, par, pa_sem.at[0])
    par_cp.start()
    acc_cp = pltpu.make_async_copy(acc_hbm, acc, pa_sem.at[1])
    acc_cp.start()

    barrier = pltpu.get_barrier_semaphore()
    for d in range(1, groups):
        pl.semaphore_signal(barrier, inc=1, device_id=((me + d) % groups,), device_id_type=MESH)
    pl.semaphore_wait(barrier, groups - 1)

    d2d = {}
    for m, t in order:
        cp = remote(grad_hbm.at[rows(m, t, 1 - core)], part.at[m, t, unit],
                    d2d_send, d2d_recv.at[m, t], partner)
        cp.start()
        d2d[m, t] = cp

    rs = {}
    slot = {}

    def rs_send_unit(m, t, phase):
        dim = ORDERS[t][phase]
        key = (m ^ dim, t, phase)
        i = slot.setdefault(key, len(slot))
        cp = remote(own.at[m, t, unit], recv.at[i, unit], rs_send, rs_recv.at[i], across[dim])
        cp.start()
        rs[key] = cp

    def rs_add(m, t, phase):
        key = (m, t, phase)
        rs[key].wait_recv()
        own[m, t, unit] = own[m, t, unit] + recv[slot[key], unit]

    for m, t in order:
        loads[m, t].wait()
        d2d[m, t].wait_recv()
        own[m, t, unit] = own[m, t, unit] + part[m, t, unit]
        if m & ORDERS[t][0]:
            rs_send_unit(m, t, 0)

    for step in range(4):
        for t, (a, b, c) in enumerate(ORDERS):
            m = (b + c, b, c, 0)[step]
            rs_add(m, t, 0)
            if m & b:
                rs_send_unit(m, t, 1)
    for step in range(2):
        for t, (a, b, c) in enumerate(ORDERS):
            m = (c, 0)[step]
            rs_add(m, t, 1)
            if m & c:
                rs_send_unit(m, t, 2)
    total = jnp.zeros((1, LANES), jnp.float32)
    for t in range(3):
        rs_add(0, t, 2)
        g = own[0, t, unit] * (1.0 / groups)
        total = total + jnp.sum(g * g, axis=0, keepdims=True)

    slots[pl.ds(me, 1)] = total
    mine = slots.at[pl.ds(me, 1)]
    for d in range(1, groups):
        remote(mine, mine, nrm_send, nrm_recv, (me + d) % groups).start()

    def wait_rows(sem, n):
        ref = full.at[pl.ds(0, n)]
        pltpu.make_async_copy(ref, ref, sem).wait()

    par_cp.wait()
    acc_cp.wait()
    wait_rows(nrm_recv, groups - 1)
    norm = jnp.sqrt(jnp.sum(slots[...]))
    norm_ref[0, 0] = norm
    scale = jnp.minimum(1.0, clip_ref[0, 0] / norm)
    rate = rate_ref[0, 0]

    ag = {}
    fwd = {}

    def ag_send_unit(m, t, phase):
        dim = ORDERS[t][2 - phase]
        r = full.at[rows(m, t, core)]
        cp = remote(r, r, ag_send, ag_recv.at[len(ag)], across[dim])
        cp.start()
        ag[m ^ dim, t] = cp

    def fwd_unit(m, t):
        r = full.at[rows(m, t, core)]
        cp = remote(r, r, fwd_send, fwd_recv.at[m, t], partner)
        cp.start()
        fwd[m, t] = cp

    for t in range(3):
        r = pl.ds(thr * t, thr)
        h = own[0, t, unit] * (1.0 / groups) * scale
        a_new = acc[r] + h * h
        newa_ref[r] = a_new
        w_new = par[r] - rate * h / (jnp.sqrt(a_new) + EPS)
        newp_ref[r] = w_new
        full[rows(0, t, core)] = w_new
        ag_send_unit(0, t, 0)
    for t in range(3):
        ag_send_unit(0, t, 1)
    for t in range(3):
        ag_send_unit(0, t, 2)
    for t in range(3):
        fwd_unit(0, t)

    def arrive(m, t):
        ag[m, t].wait_recv()

    for t, (c, b, a) in enumerate(ORDERS):
        arrive(a, t)
        ag_send_unit(a, t, 1)
        ag_send_unit(a, t, 2)
        fwd_unit(a, t)
    for k in range(2):
        for t, (c, b, a) in enumerate(ORDERS):
            m = (b, b + a)[k]
            arrive(m, t)
            ag_send_unit(m, t, 2)
            fwd_unit(m, t)
    for k in range(4):
        for t, (c, b, a) in enumerate(ORDERS):
            m = (c, c + a, c + b, c + b + a)[k]
            arrive(m, t)
            fwd_unit(m, t)

    for key in fwd:
        fwd[key].wait_recv()
    copy_ref[...] = full[...].astype(jnp.bfloat16)

    wait_rows(d2d_send, 24 * thr)
    wait_rows(rs_send, 21 * thr)
    wait_rows(nrm_send, groups - 1)
    wait_rows(ag_send, 21 * thr)
    wait_rows(fwd_send, 24 * thr)


def solution(mesh):
    groups = mesh.shape["dp"]

    def local_step(grad_row, param_blk, accum_blk, learn_rate, clip_max):
        n = grad_row.shape[1] // LANES
        blk = n // groups
        thr = blk // 3
        pad = -(-thr // 8) * 8
        f32 = jnp.float32
        vm = pl.BlockSpec(memory_space=pltpu.VMEM)
        sm = pl.BlockSpec(memory_space=pltpu.SMEM)
        hb = pl.BlockSpec(memory_space=pl.ANY)
        dma = pltpu.SemaphoreType.DMA
        newp, newa, copy, norm = pl.pallas_call(
            functools.partial(kernel, blk, thr, groups),
            out_shape=(
                jax.ShapeDtypeStruct((blk, LANES), f32),
                jax.ShapeDtypeStruct((blk, LANES), f32),
                jax.ShapeDtypeStruct((n, LANES), jnp.bfloat16),
                jax.ShapeDtypeStruct((1, 1), f32),
            ),
            in_specs=[sm, sm, hb, hb, hb],
            out_specs=(vm, vm, vm, sm),
            scratch_shapes=[
                pltpu.VMEM((8, 3, pad, LANES), f32),
                pltpu.VMEM((8, 3, pad, LANES), f32),
                pltpu.VMEM((21, pad, LANES), f32),
                pltpu.VMEM((n, LANES), f32),
                pltpu.VMEM((blk, LANES), f32),
                pltpu.VMEM((blk, LANES), f32),
                pltpu.VMEM((groups, LANES), f32),
                dma((8, 3)), dma((2,)),
                dma, dma((8, 3)), dma, dma((21,)),
                dma, dma, dma, dma((21,)), dma, dma((8, 3)),
            ],
            compiler_params=pltpu.CompilerParams(
                collective_id=0, has_side_effects=True, vmem_limit_bytes=60 * 1024 * 1024),
        )(learn_rate.reshape(1, 1), clip_max.reshape(1, 1), grad_row.reshape(n, LANES),
          param_blk.reshape(blk, LANES), accum_blk.reshape(blk, LANES))
        return newp.reshape(-1), newa.reshape(-1), copy.reshape(-1), norm.reshape(())

    return jax.shard_map(local_step, mesh=mesh, in_specs=(P("dp", None), P("dp"), P("dp"), P(), P()), out_specs=(P("dp"), P("dp"), P(), P()), check_vma=False)
```

```python
import functools
import jax
import jax.numpy as jnp
from jax import lax
from jax.sharding import PartitionSpec as P
from jax.experimental import pallas as pl
from jax.experimental.pallas import tpu as pltpu

EPS = 1e-10
LANES = 128
X, Y, Z = 1, 2, 4
ORDERS = ((X, Y, Z), (Y, Z, X), (Z, X, Y))
MESH = pl.DeviceIdType.MESH
TILES = 12


def kernel(
    blk, thr, groups,
    rate_ref, clip_ref, grad_hbm, par_hbm, acc_hbm,
    full, newa_ref, norm_ref,
    own, part, recv, par, acc, slots,
    load_sem, pa_sem, d2d_send, d2d_recv, rs_send, rs_recv,
    nrm_send, nrm_recv, ag_send, ag_recv, fwd_send, fwd_recv,
):
    me = lax.axis_index("dp")
    core = me % 2
    chip = me // 2
    x, y, z = chip % 2, (chip // 2) % 2, chip // 4
    partner = me + 1 - 2 * core
    across = {X: me + 2 - 4 * x, Y: me + 4 - 8 * y, Z: me + 8 - 16 * z}

    def base(m, c):
        xc = 1 - x if m & X else x
        yc = 1 - y if m & Y else y
        zc = 1 - z if m & Z else z
        return blk * (2 * (4 * zc + 2 * yc + xc) + c)

    def rows(m, t, c):
        return pl.ds(base(m, c) + thr * t, thr)

    unit = pl.ds(0, thr)

    def remote(src, dst, send, rcv, dev):
        return pltpu.make_async_remote_copy(
            src_ref=src, dst_ref=dst, send_sem=send, recv_sem=rcv,
            device_id=(dev,), device_id_type=MESH)

    order = []
    for pick in (
        lambda a, b, c: a + b + c, lambda a, b, c: a + b, lambda a, b, c: a + c, lambda a, b, c: a,
        lambda a, b, c: b + c, lambda a, b, c: b, lambda a, b, c: c, lambda a, b, c: 0,
    ):
        for t, dims in enumerate(ORDERS):
            order.append((pick(*dims), t))

    loads = {}
    for m, t in order:
        cp = pltpu.make_async_copy(
            grad_hbm.at[rows(m, t, core)], own.at[m, t, unit], load_sem.at[m, t])
        cp.start()
        loads[m, t] = cp
    par_cp = pltpu.make_async_copy(par_hbm, par, pa_sem.at[0])
    par_cp.start()
    acc_cp = pltpu.make_async_copy(acc_hbm, acc, pa_sem.at[1])
    acc_cp.start()

    barrier = pltpu.get_barrier_semaphore()
    for d in range(1, groups):
        pl.semaphore_signal(barrier, inc=1, device_id=((me + d) % groups,), device_id_type=MESH)
    pl.semaphore_wait(barrier, groups - 1)

    d2d = {}
    for m, t in order:
        cp = remote(grad_hbm.at[rows(m, t, 1 - core)], part.at[m, t, unit],
                    d2d_send, d2d_recv.at[m, t], partner)
        cp.start()
        d2d[m, t] = cp

    rs = {}
    slot = {}

    def rs_send_unit(m, t, phase):
        dim = ORDERS[t][phase]
        key = (m ^ dim, t, phase)
        i = slot.setdefault(key, len(slot))
        cp = remote(own.at[m, t, unit], recv.at[i, unit], rs_send, rs_recv.at[i], across[dim])
        cp.start()
        rs[key] = cp

    def rs_add(m, t, phase):
        key = (m, t, phase)
        rs[key].wait_recv()
        own[m, t, unit] = own[m, t, unit] + recv[slot[key], unit]

    for m, t in order:
        loads[m, t].wait()
        d2d[m, t].wait_recv()
        own[m, t, unit] = own[m, t, unit] + part[m, t, unit]
        if m & ORDERS[t][0]:
            rs_send_unit(m, t, 0)

    for step in range(4):
        for t, (a, b, c) in enumerate(ORDERS):
            m = (b + c, b, c, 0)[step]
            rs_add(m, t, 0)
            if m & b:
                rs_send_unit(m, t, 1)
    for step in range(2):
        for t, (a, b, c) in enumerate(ORDERS):
            m = (c, 0)[step]
            rs_add(m, t, 1)
            if m & c:
                rs_send_unit(m, t, 2)
    total = jnp.zeros((1, LANES), jnp.float32)
    for t in range(3):
        rs_add(0, t, 2)
        g = own[0, t, unit] * (1.0 / groups)
        total = total + jnp.sum(g * g, axis=0, keepdims=True)

    slots[pl.ds(me, 1)] = total
    mine = slots.at[pl.ds(me, 1)]
    for d in range(1, groups):
        remote(mine, mine, nrm_send, nrm_recv, (me + d) % groups).start()

    def wait_rows(sem, n):
        ref = full.at[pl.ds(0, n)]
        pltpu.make_async_copy(ref, ref, sem).wait()

    par_cp.wait()
    acc_cp.wait()
    wait_rows(nrm_recv, groups - 1)
    norm = jnp.sqrt(jnp.sum(slots[...]))
    norm_ref[...] = jnp.full((1, LANES), norm)
    scale = jnp.minimum(1.0, clip_ref[...] / norm)
    rate = rate_ref[...]

    ag = {}
    fwd = {}

    def ag_send_unit(m, t, phase):
        dim = ORDERS[t][2 - phase]
        r = full.at[rows(m, t, core)]
        cp = remote(r, r, ag_send, ag_recv.at[len(ag)], across[dim])
        cp.start()
        ag[m ^ dim, t] = cp

    def fwd_unit(m, t):
        r = full.at[rows(m, t, core)]
        cp = remote(r, r, fwd_send, fwd_recv.at[m, t], partner)
        cp.start()
        fwd[m, t] = cp

    for t in range(3):
        r = pl.ds(thr * t, thr)
        h = own[0, t, unit] * (1.0 / groups) * scale
        a_new = acc[r] + h * h
        newa_ref[r] = a_new
        w_new = par[r] - rate * h / (jnp.sqrt(a_new) + EPS)
        full[rows(0, t, core)] = w_new
        ag_send_unit(0, t, 0)
    for t in range(3):
        ag_send_unit(0, t, 1)
    for t in range(3):
        ag_send_unit(0, t, 2)
    for t in range(3):
        fwd_unit(0, t)

    def arrive(m, t):
        ag[m, t].wait_recv()

    for t, (c, b, a) in enumerate(ORDERS):
        arrive(a, t)
        ag_send_unit(a, t, 1)
        ag_send_unit(a, t, 2)
        fwd_unit(a, t)
    for k in range(2):
        for t, (c, b, a) in enumerate(ORDERS):
            m = (b, b + a)[k]
            arrive(m, t)
            ag_send_unit(m, t, 2)
            fwd_unit(m, t)
    for k in range(4):
        for t, (c, b, a) in enumerate(ORDERS):
            m = (c, c + a, c + b, c + b + a)[k]
            arrive(m, t)
            fwd_unit(m, t)

    for key in fwd:
        fwd[key].wait_recv()

    wait_rows(d2d_send, 24 * thr)
    wait_rows(rs_send, 21 * thr)
    wait_rows(nrm_send, groups - 1)
    wait_rows(ag_send, 21 * thr)
    wait_rows(fwd_send, 24 * thr)


def write_kernel(blk, tiles, full, newa, norm, newp_hbm, newa_hbm, copy_hbm, norm_ref, buf, sems, copy_sem):
    me = lax.axis_index("dp")
    mine = full.at[pl.ds(me * blk, blk)]
    out = [
        pltpu.make_async_copy(mine, newp_hbm, sems.at[0]),
        pltpu.make_async_copy(newa, newa_hbm, sems.at[1]),
    ]
    for cp in out:
        cp.start()
    n = full.shape[0]
    edges = [n * i // tiles // 16 * 16 for i in range(tiles)] + [n]
    for i in range(tiles):
        r = pl.ds(edges[i], edges[i + 1] - edges[i])
        buf[r] = full[r].astype(jnp.bfloat16)
        cp = pltpu.make_async_copy(buf.at[r], copy_hbm.at[r], copy_sem.at[i])
        cp.start()
        out.append(cp)
    norm_ref[...] = norm[:, :1]
    for cp in out:
        cp.wait()


def in_hbm(a):
    return pltpu.with_memory_space_constraint(a, pltpu.HBM)


def solution(mesh):
    groups = mesh.shape["dp"]

    def local_step(grad_row, param_blk, accum_blk, learn_rate, clip_max):
        n = grad_row.shape[1] // LANES
        blk = n // groups
        thr = blk // 3
        pad = -(-thr // 8) * 8
        f32 = jnp.float32
        vm = pl.BlockSpec(memory_space=pltpu.VMEM)
        sm = pl.BlockSpec(memory_space=pltpu.SMEM)
        hb = pl.BlockSpec(memory_space=pltpu.HBM)
        dma = pltpu.SemaphoreType.DMA
        full, newa, norm = pl.pallas_call(
            functools.partial(kernel, blk, thr, groups),
            out_shape=(
                pltpu.VMEM((n, LANES), f32),
                pltpu.VMEM((blk, LANES), f32),
                pltpu.VMEM((1, LANES), f32),
            ),
            in_specs=[sm, sm, hb, hb, hb],
            out_specs=(vm, vm, vm),
            scratch_shapes=[
                pltpu.VMEM((8, 3, pad, LANES), f32),
                pltpu.VMEM((8, 3, pad, LANES), f32),
                pltpu.VMEM((21, pad, LANES), f32),
                pltpu.VMEM((blk, LANES), f32),
                pltpu.VMEM((blk, LANES), f32),
                pltpu.VMEM((groups, LANES), f32),
                dma((8, 3)), dma((2,)),
                dma, dma((8, 3)), dma, dma((21,)),
                dma, dma, dma, dma((21,)), dma, dma((8, 3)),
            ],
            compiler_params=pltpu.CompilerParams(
                collective_id=0, has_side_effects=True, vmem_limit_bytes=40 * 1024 * 1024),
        )(learn_rate, clip_max, in_hbm(grad_row.reshape(n, LANES)),
          in_hbm(param_blk.reshape(blk, LANES)), in_hbm(accum_blk.reshape(blk, LANES)))
        newp, newa, copy, norm = pl.pallas_call(
            functools.partial(write_kernel, blk, TILES),
            out_shape=(
                jax.ShapeDtypeStruct((blk, LANES), f32),
                jax.ShapeDtypeStruct((blk, LANES), f32),
                jax.ShapeDtypeStruct((n, LANES), jnp.bfloat16),
                jax.ShapeDtypeStruct((1, 1), f32),
            ),
            in_specs=[vm, vm, vm],
            out_specs=(hb, hb, hb, vm),
            scratch_shapes=[
                pltpu.VMEM((n, LANES), jnp.bfloat16),
                dma((2,)), dma((TILES,)),
            ],
            compiler_params=pltpu.CompilerParams(vmem_limit_bytes=12 * 1024 * 1024),
        )(full, newa, norm)
        return newp.reshape(-1), newa.reshape(-1), copy.reshape(-1), norm.reshape(())

    return jax.shard_map(local_step, mesh=mesh, in_specs=(P("dp", None), P("dp"), P("dp"), P(), P()), out_specs=(P("dp"), P("dp"), P(), P()), check_vma=False)
```

```python
import functools
import jax
import jax.numpy as jnp
from jax import lax
from jax.sharding import PartitionSpec as P
from jax.experimental import pallas as pl
from jax.experimental.pallas import tpu as pltpu

EPS = 1e-10
LANES = 128
X, Y, Z = 1, 2, 4
ORDERS = ((X, Y, Z), (Y, Z, X), (Z, X, Y))
MESH = pl.DeviceIdType.MESH
TILES = 12
PIECES = 4


def cut(start, size, n):
    step = -(-size // (8 * n)) * 8
    return [(start + i * step, min(step, size - i * step)) for i in range(n)]


def kernel(
    blk, third, groups,
    rate_ref, clip_ref, grad_hbm, par_hbm, acc_hbm,
    full, newa_ref, norm_ref,
    own, part, recv, par, acc, slots,
    load_sem, near_sem, far_sem, nrm_sem, send_sem,
):
    me = lax.axis_index("dp")
    core = me % 2
    chip = me // 2
    x, y, z = chip % 2, (chip // 2) % 2, chip // 4
    partner = me + 1 - 2 * core
    across = {X: me + 2 - 4 * x, Y: me + 4 - 8 * y, Z: me + 8 - 16 * z}

    def base(m, c):
        xc = 1 - x if m & X else x
        yc = 1 - y if m & Y else y
        zc = 1 - z if m & Z else z
        return blk * (2 * (4 * zc + 2 * yc + xc) + c)

    thirds = [(third * t, min(third, blk - third * t)) for t in range(3)]

    def send(src, dst, kind, rcv, dev):
        pltpu.make_async_remote_copy(
            src_ref=src, dst_ref=dst, send_sem=send_sem.at[kind], recv_sem=rcv,
            device_id=(dev,), device_id_type=MESH).start()

    def wait_rows(sem, n):
        ref = full.at[pl.ds(0, n)]
        pltpu.make_async_copy(ref, ref, sem).wait()

    waves = ((X + Y + Z,), (X + Y, Y + Z, Z + X), (X, Y, Z, 0))
    for i, wave in enumerate(waves):
        for m in wave:
            pltpu.make_async_copy(
                grad_hbm.at[pl.ds(base(m, core), blk)], own.at[m, pl.ds(0, blk)], load_sem.at[i]).start()
    par_cp = pltpu.make_async_copy(par_hbm, par, load_sem.at[3])
    par_cp.start()
    acc_cp = pltpu.make_async_copy(acc_hbm, acc, load_sem.at[4])
    acc_cp.start()

    barrier = pltpu.get_barrier_semaphore()
    near = (partner, across[X], across[Y], across[Z])
    for dev in near:
        pl.semaphore_signal(barrier, inc=1, device_id=(dev,), device_id_type=MESH)
    pl.semaphore_wait(barrier, len(near))

    all_bits = X + Y + Z
    pieces = [cut(*thirds[t], PIECES) for t in range(3)]

    def exchange(m, start, size, i):
        send(grad_hbm.at[pl.ds(base(m, 1 - core) + start, size)],
             part.at[m, pl.ds(start, size)], 0, near_sem.at[i], partner)

    for p in range(PIECES):
        for t in range(3):
            exchange(all_bits, *pieces[t][p], p)
    for i in (1, 2):
        for m in waves[i]:
            exchange(m, 0, blk, PIECES - 1 + i)

    def fold(m, start, size):
        r = pl.ds(start, size)
        own[m, r] = own[m, r] + part[m, r]

    def unit(step, t):
        a, b, c = ORDERS[t]
        return (b + c, b, c, 0, c, 0, 0)[step]

    PHASE = (0, 0, 0, 0, 1, 1, 2)

    def push(step, t, start, size):
        dim = ORDERS[t][PHASE[step]]
        s0 = thirds[t][0]
        send(own.at[unit(step, t) ^ dim, pl.ds(start, size)],
             recv.at[3 * step + t, pl.ds(start - s0, size)], 1, far_sem.at[step], across[dim])

    load_waits = [len(w) * blk for w in waves]
    wait_rows(load_sem.at[0], load_waits[0])
    for p in range(PIECES):
        wait_rows(near_sem.at[p], sum(pieces[t][p][1] for t in range(3)))
        for t in range(3):
            fold(all_bits, *pieces[t][p])
            push(0, t, *pieces[t][p])
    wait_rows(load_sem.at[1], load_waits[1])
    wait_rows(near_sem.at[PIECES], load_waits[1])
    for step in (1, 2):
        for t in range(3):
            fold(unit(step, t) ^ ORDERS[t][0], *thirds[t])
            push(step, t, *thirds[t])
    wait_rows(load_sem.at[2], load_waits[2])
    wait_rows(near_sem.at[PIECES + 1], load_waits[2])
    for t in range(3):
        fold(unit(3, t) ^ ORDERS[t][0], *thirds[t])
        push(3, t, *thirds[t])
    for step in range(4):
        for t in range(3):
            fold(unit(step, t), *thirds[t])

    total = jnp.zeros((1, LANES), jnp.float32)
    for step in range(7):
        wait_rows(far_sem.at[step], blk)
        for t in range(3):
            m = unit(step, t)
            s0, size = thirds[t]
            got = own[m, pl.ds(s0, size)] + recv[3 * step + t, pl.ds(0, size)]
            own[m, pl.ds(s0, size)] = got
            if step in (0, 1):
                push(4 + step, t, *thirds[t])
            if step == 4:
                push(6, t, *thirds[t])
            if step == 6:
                g = got * (1.0 / groups)
                total = total + jnp.sum(g * g, axis=0, keepdims=True)

    slots[pl.ds(me, 1)] = total
    mine = slots.at[pl.ds(me, 1)]
    for d in range(1, groups):
        send(mine, mine, 2, nrm_sem, (me + d) % groups)
    par_cp.wait()
    acc_cp.wait()
    wait_rows(nrm_sem, groups - 1)
    square = jnp.sum(jnp.sum(slots[...], axis=0, keepdims=True), axis=1, keepdims=True)
    norm = jnp.sqrt(square)
    norm_ref[...] = norm
    scale = jnp.minimum(1.0, clip_ref[...] / norm)
    rate = rate_ref[...]

    def rows(m, start, size):
        return full.at[pl.ds(base(m, core) + start, size)]

    def gather(m, t, j, rcv, start, size):
        send(rows(m, start, size), rows(m, start, size), 3, rcv, across[ORDERS[t][2 - j]])

    def forward(m, start, size):
        send(rows(m, start, size), rows(m, start, size), 4, near_sem.at[PIECES], partner)

    for p in range(PIECES):
        for t in range(3):
            start, size = pieces[t][p]
            r = pl.ds(start, size)
            h = own[0, r] * (1.0 / groups) * scale
            a_new = acc[r] + h * h
            newa_ref[r] = a_new
            full[pl.ds(base(0, core) + start, size)] = par[r] - rate * h / (jnp.sqrt(a_new) + EPS)
            gather(0, t, 0, far_sem.at[0], start, size)
    for j in (1, 2):
        for t in range(3):
            gather(0, t, j, far_sem.at[j], *thirds[t])
    forward(0, 0, blk)

    for step in range(6):
        wait_rows(far_sem.at[step], blk)
        for t in range(3):
            c, b, a = ORDERS[t]
            m = (a, b, c, a + b, a + c, b + c)[step]
            if step == 0:
                gather(m, t, 1, far_sem.at[3], *thirds[t])
            if step in (0, 1):
                gather(m, t, 2, far_sem.at[4 + step], *thirds[t])
            if step == 3:
                for p in range(PIECES):
                    gather(m, t, 2, near_sem.at[p], *pieces[t][p])
        for t in range(3):
            c, b, a = ORDERS[t]
            forward((a, b, c, a + b, a + c, b + c)[step], *thirds[t])
    for p in range(PIECES):
        wait_rows(near_sem.at[p], sum(pieces[t][p][1] for t in range(3)))
        for t in range(3):
            forward(all_bits, *pieces[t][p])
    wait_rows(near_sem.at[PIECES], 8 * blk)

    for kind, n in enumerate((8 * blk, 7 * blk, groups - 1, 7 * blk, 8 * blk)):
        wait_rows(send_sem.at[kind], n)


def write_kernel(blk, full, newa, norm, newp_hbm, newa_hbm, copy_hbm, norm_hbm, buf, sems):
    me = lax.axis_index("dp")
    mine = full.at[pl.ds(me * blk, blk)]
    out = [
        pltpu.make_async_copy(mine, newp_hbm, sems.at[0]),
        pltpu.make_async_copy(newa, newa_hbm, sems.at[1]),
        pltpu.make_async_copy(norm, norm_hbm, sems.at[2]),
    ]
    for cp in out:
        cp.start()
    n = full.shape[0]
    edges = [n * i // TILES // 16 * 16 for i in range(TILES)] + [n]
    for i in range(TILES):
        r = pl.ds(edges[i], edges[i + 1] - edges[i])
        buf[r] = full[r].astype(jnp.bfloat16)
        pltpu.make_async_copy(buf.at[r], copy_hbm.at[r], sems.at[3]).start()
    pltpu.make_async_copy(buf, copy_hbm, sems.at[3]).wait()
    for cp in out:
        cp.wait()


def in_hbm(a):
    return pltpu.with_memory_space_constraint(a, pltpu.HBM)


def solution(mesh):
    groups = mesh.shape["dp"]

    def local_step(grad_row, param_blk, accum_blk, learn_rate, clip_max):
        n = grad_row.shape[1] // LANES
        blk = n // groups
        third = -(-blk // 24) * 8
        pad = -(-blk // 8) * 8
        f32 = jnp.float32
        vm = pl.BlockSpec(memory_space=pltpu.VMEM)
        sm = pl.BlockSpec(memory_space=pltpu.SMEM)
        hb = pl.BlockSpec(memory_space=pltpu.HBM)
        dma = pltpu.SemaphoreType.DMA
        full, newa, norm = pl.pallas_call(
            functools.partial(kernel, blk, third, groups),
            out_shape=(
                pltpu.VMEM((n, LANES), f32),
                pltpu.VMEM((blk, LANES), f32),
                pltpu.VMEM((1, 1), f32),
            ),
            in_specs=[sm, sm, hb, hb, hb],
            out_specs=(vm, vm, vm),
            scratch_shapes=[
                pltpu.VMEM((8, pad, LANES), f32),
                pltpu.VMEM((8, pad, LANES), f32),
                pltpu.VMEM((21, third, LANES), f32),
                pltpu.VMEM((blk, LANES), f32),
                pltpu.VMEM((blk, LANES), f32),
                pltpu.VMEM((groups, LANES), f32),
                dma((5,)), dma((PIECES + 2,)), dma((7,)), dma, dma((5,)),
            ],
            compiler_params=pltpu.CompilerParams(
                collective_id=0, has_side_effects=True, vmem_limit_bytes=40 * 1024 * 1024),
        )(learn_rate, clip_max, in_hbm(grad_row.reshape(n, LANES)),
          in_hbm(param_blk.reshape(blk, LANES)), in_hbm(accum_blk.reshape(blk, LANES)))
        newp, newa, copy, norm = pl.pallas_call(
            functools.partial(write_kernel, blk),
            out_shape=(
                jax.ShapeDtypeStruct((blk, LANES), f32),
                jax.ShapeDtypeStruct((blk, LANES), f32),
                jax.ShapeDtypeStruct((n, LANES), jnp.bfloat16),
                jax.ShapeDtypeStruct((1, 1), f32),
            ),
            in_specs=[vm, vm, vm],
            out_specs=(hb, hb, hb, hb),
            scratch_shapes=[pltpu.VMEM((n, LANES), jnp.bfloat16), dma((4,))],
            compiler_params=pltpu.CompilerParams(vmem_limit_bytes=12 * 1024 * 1024),
        )(full, newa, norm)
        return newp.reshape(-1), newa.reshape(-1), copy.reshape(-1), norm.reshape(())

    return jax.shard_map(local_step, mesh=mesh, in_specs=(P("dp", None), P("dp"), P("dp"), P(), P()), out_specs=(P("dp"), P("dp"), P(), P()), check_vma=False)
```

```python
import functools
import jax
import jax.numpy as jnp
from jax import lax
from jax.sharding import PartitionSpec as P
from jax.experimental import pallas as pl
from jax.experimental.pallas import tpu as pltpu

EPS = 1e-10
LANES = 128
X, Y, Z = 1, 2, 4
ORDERS = ((X, Y, Z), (Y, Z, X), (Z, X, Y))
MESH = pl.DeviceIdType.MESH
TILES = 12
PIECES = 4


def cut(start, size, n):
    step = -(-size // (8 * n)) * 8
    return [(start + i * step, min(step, size - i * step)) for i in range(n)]


def kernel(
    blk, third, groups,
    rate_ref, clip_ref, grad_hbm, par_hbm, acc_hbm,
    full, newa_ref, norm_ref,
    own, part, recv, par, acc, slots,
    load_sem, near_sem, far_sem, nrm_sem, send_sem,
):
    me = lax.axis_index("dp")
    core = me % 2
    chip = me // 2
    x, y, z = chip % 2, (chip // 2) % 2, chip // 4
    partner = me + 1 - 2 * core
    across = {X: me + 2 - 4 * x, Y: me + 4 - 8 * y, Z: me + 8 - 16 * z}

    def place(m, c):
        xc = 1 - x if m & X else x
        yc = 1 - y if m & Y else y
        zc = 1 - z if m & Z else z
        return 2 * (4 * zc + 2 * yc + xc) + c

    def base(m, c):
        return blk * place(m, c)

    thirds = [(third * t, min(third, blk - third * t)) for t in range(3)]

    def send(src, dst, kind, rcv, dev):
        pltpu.make_async_remote_copy(
            src_ref=src, dst_ref=dst, send_sem=send_sem.at[kind], recv_sem=rcv,
            device_id=(dev,), device_id_type=MESH).start()

    def wait_rows(sem, n):
        ref = full.at[pl.ds(0, n)]
        pltpu.make_async_copy(ref, ref, sem).wait()

    waves = ((X + Y + Z,), (X + Y, Y + Z, Z + X), (X, Y, Z, 0))
    for i, wave in enumerate(waves):
        for m in wave:
            pltpu.make_async_copy(
                grad_hbm.at[pl.ds(base(m, core), blk)], own.at[m, pl.ds(0, blk)], load_sem.at[i]).start()
    par_cp = pltpu.make_async_copy(par_hbm, par, load_sem.at[3])
    par_cp.start()
    acc_cp = pltpu.make_async_copy(acc_hbm, acc, load_sem.at[4])
    acc_cp.start()

    barrier = pltpu.get_barrier_semaphore()
    near = (partner, across[X], across[Y], across[Z])
    for dev in near:
        pl.semaphore_signal(barrier, inc=1, device_id=(dev,), device_id_type=MESH)
    pl.semaphore_wait(barrier, len(near))

    all_bits = X + Y + Z
    pieces = [cut(*thirds[t], PIECES) for t in range(3)]

    def exchange(m, start, size, i):
        send(grad_hbm.at[pl.ds(base(m, 1 - core) + start, size)],
             part.at[m, pl.ds(start, size)], 0, near_sem.at[i], partner)

    for p in range(PIECES):
        for t in range(3):
            exchange(all_bits, *pieces[t][p], p)
    for i in (1, 2):
        for m in waves[i]:
            exchange(m, 0, blk, PIECES - 1 + i)

    def fold(m, start, size):
        r = pl.ds(start, size)
        own[m, r] = own[m, r] + part[m, r]

    def unit(step, t):
        a, b, c = ORDERS[t]
        return (b + c, b, c, 0, c, 0, 0)[step]

    PHASE = (0, 0, 0, 0, 1, 1, 2)

    def push(step, t, start, size):
        dim = ORDERS[t][PHASE[step]]
        s0 = thirds[t][0]
        send(own.at[unit(step, t) ^ dim, pl.ds(start, size)],
             recv.at[3 * step + t, pl.ds(start - s0, size)], 1, far_sem.at[step], across[dim])

    load_waits = [len(w) * blk for w in waves]
    wait_rows(load_sem.at[0], load_waits[0])
    for p in range(PIECES):
        wait_rows(near_sem.at[p], sum(pieces[t][p][1] for t in range(3)))
        for t in range(3):
            fold(all_bits, *pieces[t][p])
            push(0, t, *pieces[t][p])
    wait_rows(load_sem.at[1], load_waits[1])
    wait_rows(near_sem.at[PIECES], load_waits[1])
    for step in (1, 2):
        for t in range(3):
            fold(unit(step, t) ^ ORDERS[t][0], *thirds[t])
            push(step, t, *thirds[t])
    wait_rows(load_sem.at[2], load_waits[2])
    wait_rows(near_sem.at[PIECES + 1], load_waits[2])
    for t in range(3):
        fold(unit(3, t) ^ ORDERS[t][0], *thirds[t])
        push(3, t, *thirds[t])
    for step in range(4):
        for t in range(3):
            fold(unit(step, t), *thirds[t])

    total = jnp.zeros((1, LANES), jnp.float32)
    for step in range(7):
        wait_rows(far_sem.at[step], blk)
        for t in range(3):
            m = unit(step, t)
            s0, size = thirds[t]
            got = own[m, pl.ds(s0, size)] + recv[3 * step + t, pl.ds(0, size)]
            own[m, pl.ds(s0, size)] = got
            if step in (0, 1):
                push(4 + step, t, *thirds[t])
            if step == 4:
                push(6, t, *thirds[t])
            if step == 6:
                g = got * (1.0 / groups)
                total = total + jnp.sum(g * g, axis=0, keepdims=True)

    slots[pl.ds(me, 1)] = total
    mine = slots.at[pl.ds(me, 1)]
    for m in (7, 3, 6, 5, 1, 2, 4):
        for c in (core, 1 - core):
            send(mine, mine, 2, nrm_sem, place(m, c))
    send(mine, mine, 2, nrm_sem, partner)
    par_cp.wait()
    acc_cp.wait()
    wait_rows(nrm_sem, groups - 1)
    square = jnp.sum(jnp.sum(slots[...], axis=0, keepdims=True), axis=1, keepdims=True)
    norm = jnp.sqrt(square)
    norm_ref[...] = jnp.broadcast_to(norm, (1, LANES))
    scale = jnp.minimum(1.0, clip_ref[...] / norm)
    rate = rate_ref[...]

    def rows(m, start, size, c=core):
        return full.at[pl.ds(base(m, c) + start, size)]

    def gather(m, t, j, rcv, start, size):
        send(rows(m, start, size), rows(m, start, size), 3, rcv, across[ORDERS[t][2 - j]])

    def forward(m, start, size, c=core):
        send(rows(m, start, size, c), rows(m, start, size, c), 4, near_sem.at[PIECES], partner)

    for p in range(PIECES):
        for t in range(3):
            start, size = pieces[t][p]
            r = pl.ds(start, size)
            h = own[0, r] * (1.0 / groups) * scale
            a_new = acc[r] + h * h
            newa_ref[r] = a_new
            full[pl.ds(base(0, core) + start, size)] = par[r] - rate * h / (jnp.sqrt(a_new) + EPS)
            gather(0, t, 0, far_sem.at[0], start, size)
    for j in (1, 2):
        for t in range(3):
            gather(0, t, j, far_sem.at[j], *thirds[t])
    forward(0, 0, blk)

    for step in range(6):
        wait_rows(far_sem.at[step], blk)
        for t in range(3):
            c, b, a = ORDERS[t]
            m = (a, b, c, a + b, a + c, b + c)[step]
            if step == 0:
                gather(m, t, 1, far_sem.at[3], *thirds[t])
            if step in (0, 1):
                gather(m, t, 2, far_sem.at[4 + step], *thirds[t])
            if step == 3:
                for p in range(PIECES):
                    r = rows(m, *pieces[t][p])
                    send(r, r, 3, near_sem.at[p], place(ORDERS[t][0], 1 - core))
        for t in range(3):
            c, b, a = ORDERS[t]
            forward((a, b, c, a + b, a + c, b + c)[step], *thirds[t])
    for p in range(PIECES):
        wait_rows(near_sem.at[p], sum(pieces[t][p][1] for t in range(3)))
        for t in range(3):
            forward(all_bits, *pieces[t][p], 1 - core)
    wait_rows(near_sem.at[PIECES], 8 * blk)

    for kind, n in enumerate((8 * blk, 7 * blk, groups - 1, 7 * blk, 8 * blk)):
        wait_rows(send_sem.at[kind], n)


def write_kernel(blk, full, newa, norm, newp_hbm, newa_hbm, copy_hbm, norm_hbm, buf, one, sems):
    me = lax.axis_index("dp")
    mine = full.at[pl.ds(me * blk, blk)]
    one[...] = norm[:, :1]
    out = [
        pltpu.make_async_copy(mine, newp_hbm, sems.at[0]),
        pltpu.make_async_copy(newa, newa_hbm, sems.at[1]),
        pltpu.make_async_copy(one, norm_hbm, sems.at[2]),
    ]
    for cp in out:
        cp.start()
    n = full.shape[0]
    edges = [n * i // TILES // 16 * 16 for i in range(TILES)] + [n]
    for i in range(TILES):
        r = pl.ds(edges[i], edges[i + 1] - edges[i])
        buf[r] = full[r].astype(jnp.bfloat16)
        pltpu.make_async_copy(buf.at[r], copy_hbm.at[r], sems.at[3]).start()
    pltpu.make_async_copy(buf, copy_hbm, sems.at[3]).wait()
    for cp in out:
        cp.wait()


def in_hbm(a):
    return pltpu.with_memory_space_constraint(a, pltpu.HBM)


def solution(mesh):
    groups = mesh.shape["dp"]

    def local_step(grad_row, param_blk, accum_blk, learn_rate, clip_max):
        n = grad_row.shape[1] // LANES
        blk = n // groups
        third = -(-blk // 24) * 8
        pad = -(-blk // 8) * 8
        f32 = jnp.float32
        vm = pl.BlockSpec(memory_space=pltpu.VMEM)
        sm = pl.BlockSpec(memory_space=pltpu.SMEM)
        hb = pl.BlockSpec(memory_space=pltpu.HBM)
        dma = pltpu.SemaphoreType.DMA
        full, newa, norm = pl.pallas_call(
            functools.partial(kernel, blk, third, groups),
            out_shape=(
                pltpu.VMEM((n, LANES), f32),
                pltpu.VMEM((blk, LANES), f32),
                pltpu.VMEM((1, LANES), f32),
            ),
            in_specs=[sm, sm, hb, hb, hb],
            out_specs=(vm, vm, vm),
            scratch_shapes=[
                pltpu.VMEM((8, pad, LANES), f32),
                pltpu.VMEM((8, pad, LANES), f32),
                pltpu.VMEM((21, third, LANES), f32),
                pltpu.VMEM((blk, LANES), f32),
                pltpu.VMEM((blk, LANES), f32),
                pltpu.VMEM((groups, LANES), f32),
                dma((5,)), dma((PIECES + 2,)), dma((7,)), dma, dma((5,)),
            ],
            compiler_params=pltpu.CompilerParams(
                collective_id=0, has_side_effects=True, vmem_limit_bytes=40 * 1024 * 1024),
        )(learn_rate, clip_max, in_hbm(grad_row.reshape(n, LANES)),
          in_hbm(param_blk.reshape(blk, LANES)), in_hbm(accum_blk.reshape(blk, LANES)))
        newp, newa, copy, norm = pl.pallas_call(
            functools.partial(write_kernel, blk),
            out_shape=(
                jax.ShapeDtypeStruct((blk, LANES), f32),
                jax.ShapeDtypeStruct((blk, LANES), f32),
                jax.ShapeDtypeStruct((n, LANES), jnp.bfloat16),
                jax.ShapeDtypeStruct((1, 1), f32),
            ),
            in_specs=[vm, vm, vm],
            out_specs=(hb, hb, hb, hb),
            scratch_shapes=[pltpu.VMEM((n, LANES), jnp.bfloat16), pltpu.VMEM((1, 1), f32), dma((4,))],
            compiler_params=pltpu.CompilerParams(vmem_limit_bytes=12 * 1024 * 1024),
        )(full, newa, norm)
        return newp.reshape(-1), newa.reshape(-1), copy.reshape(-1), norm.reshape(())

    return jax.shard_map(local_step, mesh=mesh, in_specs=(P("dp", None), P("dp"), P("dp"), P(), P()), out_specs=(P("dp"), P("dp"), P(), P()), check_vma=False)
```

```python
import functools
import jax
import jax.numpy as jnp
from jax import lax
from jax.sharding import PartitionSpec as P
from jax.experimental import pallas as pl
from jax.experimental.pallas import tpu as pltpu

EPS = 1e-10
LANES = 128
X, Y, Z = 1, 2, 4
ORDERS = ((X, Y, Z), (Y, Z, X), (Z, X, Y))
MESH = pl.DeviceIdType.MESH
TILES = 12
PIECES = 4


def cut(start, size, n):
    step = -(-size // (8 * n)) * 8
    return [(start + i * step, min(step, size - i * step)) for i in range(n)]


def kernel(
    blk, third, groups,
    rate_ref, clip_ref, grad_hbm, par_hbm, acc_hbm,
    full, newa_ref, norm_ref,
    own, part, recv, par, acc, slots, raw,
    load_sem, near_sem, far_sem, nrm_sem, raw_sem, send_sem,
):
    me = lax.axis_index("dp")
    core = me % 2
    chip = me // 2
    x, y, z = chip % 2, (chip // 2) % 2, chip // 4
    partner = me + 1 - 2 * core
    across = {X: me + 2 - 4 * x, Y: me + 4 - 8 * y, Z: me + 8 - 16 * z}

    def place(m, c):
        xc = 1 - x if m & X else x
        yc = 1 - y if m & Y else y
        zc = 1 - z if m & Z else z
        return 2 * (4 * zc + 2 * yc + xc) + c

    def base(m, c):
        return blk * place(m, c)

    thirds = [(third * t, min(third, blk - third * t)) for t in range(3)]

    def send(src, dst, kind, rcv, dev):
        pltpu.make_async_remote_copy(
            src_ref=src, dst_ref=dst, send_sem=send_sem.at[kind], recv_sem=rcv,
            device_id=(dev,), device_id_type=MESH).start()

    def wait_rows(sem, n):
        ref = full.at[pl.ds(0, n)]
        pltpu.make_async_copy(ref, ref, sem).wait()

    waves = ((X + Y + Z,), (X + Y, Y + Z, Z + X), (X, Y, Z, 0))
    for i, wave in enumerate(waves):
        for m in wave:
            pltpu.make_async_copy(
                grad_hbm.at[pl.ds(base(m, core), blk)], own.at[m, pl.ds(0, blk)], load_sem.at[i]).start()
    par_cp = pltpu.make_async_copy(par_hbm, par, load_sem.at[3])
    par_cp.start()
    acc_cp = pltpu.make_async_copy(acc_hbm, acc, load_sem.at[4])
    acc_cp.start()

    barrier = pltpu.get_barrier_semaphore()
    near = (partner, across[X], across[Y], across[Z])
    for dev in near:
        pl.semaphore_signal(barrier, inc=1, device_id=(dev,), device_id_type=MESH)
    pl.semaphore_wait(barrier, len(near))

    all_bits = X + Y + Z
    pieces = [cut(*thirds[t], PIECES) for t in range(3)]

    def exchange(m, start, size, i):
        send(grad_hbm.at[pl.ds(base(m, 1 - core) + start, size)],
             part.at[m, pl.ds(start, size)], 0, near_sem.at[i], partner)

    for p in range(PIECES):
        for t in range(3):
            exchange(all_bits, *pieces[t][p], p)
    for i in (1, 2):
        for m in waves[i]:
            exchange(m, 0, blk, PIECES - 1 + i)

    def fold(m, start, size):
        r = pl.ds(start, size)
        own[m, r] = own[m, r] + part[m, r]

    def unit(step, t):
        a, b, c = ORDERS[t]
        return (b + c, b, c, 0, c, 0, 0)[step]

    PHASE = (0, 0, 0, 0, 1, 1, 2)

    def push(step, t, start, size):
        dim = ORDERS[t][PHASE[step]]
        s0 = thirds[t][0]
        send(own.at[unit(step, t) ^ dim, pl.ds(start, size)],
             recv.at[3 * step + t, pl.ds(start - s0, size)], 1, far_sem.at[step], across[dim])

    load_waits = [len(w) * blk for w in waves]
    wait_rows(load_sem.at[0], load_waits[0])
    for p in range(PIECES):
        wait_rows(near_sem.at[p], sum(pieces[t][p][1] for t in range(3)))
        for t in range(3):
            fold(all_bits, *pieces[t][p])
            push(0, t, *pieces[t][p])
    wait_rows(load_sem.at[1], load_waits[1])
    wait_rows(near_sem.at[PIECES], load_waits[1])
    for step in (1, 2):
        for t in range(3):
            fold(unit(step, t) ^ ORDERS[t][0], *thirds[t])
            push(step, t, *thirds[t])
    wait_rows(load_sem.at[2], load_waits[2])
    wait_rows(near_sem.at[PIECES + 1], load_waits[2])
    for t in range(3):
        fold(unit(3, t) ^ ORDERS[t][0], *thirds[t])
        push(3, t, *thirds[t])
    for step in range(4):
        for t in range(3):
            fold(unit(step, t), *thirds[t])

    def early(t, k, src):
        start, size = pieces[t][0]
        send(src.at[pl.ds(start, size)], raw.at[3 * t + k, pl.ds(0, size)], 5, raw_sem, across[ORDERS[t][2]])

    n_raw = 3 * sum(pieces[t][0][1] for t in range(3))
    par_cp.wait()
    acc_cp.wait()
    total = jnp.zeros((1, LANES), jnp.float32)
    for step in range(7):
        wait_rows(far_sem.at[step], blk)
        for t in range(3):
            m = unit(step, t)
            s0, size = thirds[t]
            got = own[m, pl.ds(s0, size)] + recv[3 * step + t, pl.ds(0, size)]
            own[m, pl.ds(s0, size)] = got
            if step in (0, 1):
                push(4 + step, t, *thirds[t])
            if step == 4:
                push(6, t, *thirds[t])
            if step == 6:
                g = got * (1.0 / groups)
                total = total + jnp.sum(g * g, axis=0, keepdims=True)
        if step == 4:
            for t in range(3):
                early(t, 0, par)
                early(t, 1, acc)

    slots[pl.ds(me, 1)] = total
    mine = slots.at[pl.ds(me, 1)]
    for m in (7, 3, 6, 5, 1, 2, 4):
        for c in (core, 1 - core):
            send(mine, mine, 2, nrm_sem, place(m, c))
    send(mine, mine, 2, nrm_sem, partner)
    for t in range(3):
        early(t, 2, own.at[0])
    wait_rows(nrm_sem, groups - 1)
    square = jnp.sum(jnp.sum(slots[...], axis=0, keepdims=True), axis=1, keepdims=True)
    norm = jnp.sqrt(square)
    norm_ref[...] = jnp.broadcast_to(norm, (1, LANES))
    scale = jnp.minimum(1.0, clip_ref[...] / norm)
    rate = rate_ref[...]

    def rows(m, start, size, c=core):
        return full.at[pl.ds(base(m, c) + start, size)]

    def gather(m, t, j, rcv, start, size):
        send(rows(m, start, size), rows(m, start, size), 3, rcv, across[ORDERS[t][2 - j]])

    def forward(m, start, size, c=core):
        send(rows(m, start, size, c), rows(m, start, size, c), 4, near_sem.at[PIECES], partner)

    def update(w, a, total):
        h = total * (1.0 / groups) * scale
        a_new = a + h * h
        return a_new, w - rate * h / (jnp.sqrt(a_new) + EPS)

    for p in (*range(1, PIECES), 0):
        for t in range(3):
            start, size = pieces[t][p]
            r = pl.ds(start, size)
            newa_ref[r], full[pl.ds(base(0, core) + start, size)] = update(par[r], acc[r], own[0, r])
            if p:
                gather(0, t, 0, far_sem.at[0], start, size)
    for j in (1, 2):
        for t in range(3):
            gather(0, t, j, far_sem.at[j], *thirds[t])
    forward(0, 0, blk)
    wait_rows(raw_sem, n_raw)
    for t in range(3):
        start, size = pieces[t][0]
        r = pl.ds(0, size)
        full[pl.ds(base(ORDERS[t][2], core) + start, size)] = update(
            raw[3 * t, r], raw[3 * t + 1, r], raw[3 * t + 2, r])[1]

    for step in range(6):
        wait_rows(far_sem.at[step], blk if step else blk - n_raw // 3)
        for t in range(3):
            c, b, a = ORDERS[t]
            m = (a, b, c, a + b, a + c, b + c)[step]
            if step == 0:
                gather(m, t, 1, far_sem.at[3], *thirds[t])
            if step in (0, 1):
                gather(m, t, 2, far_sem.at[4 + step], *thirds[t])
            if step == 3:
                for p in range(PIECES):
                    r = rows(m, *pieces[t][p])
                    send(r, r, 3, near_sem.at[p], place(ORDERS[t][0], 1 - core))
        for t in range(3):
            c, b, a = ORDERS[t]
            forward((a, b, c, a + b, a + c, b + c)[step], *thirds[t])
    for p in range(PIECES):
        wait_rows(near_sem.at[p], sum(pieces[t][p][1] for t in range(3)))
        for t in range(3):
            forward(all_bits, *pieces[t][p], 1 - core)
    wait_rows(near_sem.at[PIECES], 8 * blk)

    for kind, n in enumerate((8 * blk, 7 * blk, groups - 1, 7 * blk - n_raw // 3, 8 * blk, n_raw)):
        wait_rows(send_sem.at[kind], n)


def write_kernel(blk, full, newa, norm, newp_hbm, newa_hbm, copy_hbm, norm_hbm, buf, one, sems):
    me = lax.axis_index("dp")
    mine = full.at[pl.ds(me * blk, blk)]
    one[...] = norm[:, :1]
    out = [
        pltpu.make_async_copy(mine, newp_hbm, sems.at[0]),
        pltpu.make_async_copy(newa, newa_hbm, sems.at[1]),
        pltpu.make_async_copy(one, norm_hbm, sems.at[2]),
    ]
    for cp in out:
        cp.start()
    n = full.shape[0]
    edges = [n * i // TILES // 16 * 16 for i in range(TILES)] + [n]
    for i in range(TILES):
        r = pl.ds(edges[i], edges[i + 1] - edges[i])
        buf[r] = full[r].astype(jnp.bfloat16)
        pltpu.make_async_copy(buf.at[r], copy_hbm.at[r], sems.at[3]).start()
    pltpu.make_async_copy(buf, copy_hbm, sems.at[3]).wait()
    for cp in out:
        cp.wait()


def in_hbm(a):
    return pltpu.with_memory_space_constraint(a, pltpu.HBM)


def solution(mesh):
    groups = mesh.shape["dp"]

    def local_step(grad_row, param_blk, accum_blk, learn_rate, clip_max):
        n = grad_row.shape[1] // LANES
        blk = n // groups
        third = -(-blk // 24) * 8
        pad = -(-blk // 8) * 8
        f32 = jnp.float32
        vm = pl.BlockSpec(memory_space=pltpu.VMEM)
        sm = pl.BlockSpec(memory_space=pltpu.SMEM)
        hb = pl.BlockSpec(memory_space=pltpu.HBM)
        dma = pltpu.SemaphoreType.DMA
        full, newa, norm = pl.pallas_call(
            functools.partial(kernel, blk, third, groups),
            out_shape=(
                pltpu.VMEM((n, LANES), f32),
                pltpu.VMEM((blk, LANES), f32),
                pltpu.VMEM((1, LANES), f32),
            ),
            in_specs=[sm, sm, hb, hb, hb],
            out_specs=(vm, vm, vm),
            scratch_shapes=[
                pltpu.VMEM((8, pad, LANES), f32),
                pltpu.VMEM((8, pad, LANES), f32),
                pltpu.VMEM((21, third, LANES), f32),
                pltpu.VMEM((blk, LANES), f32),
                pltpu.VMEM((blk, LANES), f32),
                pltpu.VMEM((groups, LANES), f32),
                pltpu.VMEM((9, third, LANES), f32),
                dma((5,)), dma((PIECES + 2,)), dma((7,)), dma, dma, dma((6,)),
            ],
            compiler_params=pltpu.CompilerParams(
                collective_id=0, has_side_effects=True, vmem_limit_bytes=40 * 1024 * 1024),
        )(learn_rate, clip_max, in_hbm(grad_row.reshape(n, LANES)),
          in_hbm(param_blk.reshape(blk, LANES)), in_hbm(accum_blk.reshape(blk, LANES)))
        newp, newa, copy, norm = pl.pallas_call(
            functools.partial(write_kernel, blk),
            out_shape=(
                jax.ShapeDtypeStruct((blk, LANES), f32),
                jax.ShapeDtypeStruct((blk, LANES), f32),
                jax.ShapeDtypeStruct((n, LANES), jnp.bfloat16),
                jax.ShapeDtypeStruct((1, 1), f32),
            ),
            in_specs=[vm, vm, vm],
            out_specs=(hb, hb, hb, hb),
            scratch_shapes=[pltpu.VMEM((n, LANES), jnp.bfloat16), pltpu.VMEM((1, 1), f32), dma((4,))],
            compiler_params=pltpu.CompilerParams(vmem_limit_bytes=12 * 1024 * 1024),
        )(full, newa, norm)
        return newp.reshape(-1), newa.reshape(-1), copy.reshape(-1), norm.reshape(())

    return jax.shard_map(local_step, mesh=mesh, in_specs=(P("dp", None), P("dp"), P("dp"), P(), P()), out_specs=(P("dp"), P("dp"), P(), P()), check_vma=False)
```

```python
import functools
import jax
import jax.numpy as jnp
from jax import lax
from jax.sharding import PartitionSpec as P
from jax.experimental import pallas as pl
from jax.experimental.pallas import tpu as pltpu

EPS = 1e-10
LANES = 128
X, Y, Z = 1, 2, 4
ORDERS = ((X, Y, Z), (Y, Z, X), (Z, X, Y))
MESH = pl.DeviceIdType.MESH
TILES = 12
PIECES = 6
AHEAD = 104
EARLY = 160
BOTH = 112
FIRST = 64


def cut(start, size, n):
    step = -(-size // (8 * n)) * 8
    return [(start + i * step, min(step, size - i * step)) for i in range(n)]


def kernel(
    blk, third, groups,
    rate_ref, clip_ref, grad_hbm, par_hbm, acc_hbm,
    full, newa_ref, norm_ref,
    own, part, recv, other, par, acc, slots, raw,
    load_sem, near_sem, far_sem, nrm_sem, raw_sem, send_sem,
):
    me = lax.axis_index("dp")
    core = me % 2
    chip = me // 2
    x, y, z = chip % 2, (chip // 2) % 2, chip // 4
    partner = me + 1 - 2 * core
    across = {X: me + 2 - 4 * x, Y: me + 4 - 8 * y, Z: me + 8 - 16 * z}

    def place(m, c):
        xc = 1 - x if m & X else x
        yc = 1 - y if m & Y else y
        zc = 1 - z if m & Z else z
        return 2 * (4 * zc + 2 * yc + xc) + c

    def base(m, c):
        return blk * place(m, c)

    thirds = [(third * t, min(third, blk - third * t)) for t in range(3)]

    def send(src, dst, kind, rcv, dev):
        pltpu.make_async_remote_copy(
            src_ref=src, dst_ref=dst, send_sem=send_sem.at[kind], recv_sem=rcv,
            device_id=(dev,), device_id_type=MESH).start()

    def wait_rows(sem, n):
        ref = full.at[pl.ds(0, n)]
        pltpu.make_async_copy(ref, ref, sem).wait()

    waves = ((X + Y + Z,), (X + Y, Y + Z, Z + X), (X, Y, Z, 0))
    for i, wave in enumerate(waves):
        for m in wave:
            pltpu.make_async_copy(
                grad_hbm.at[pl.ds(base(m, core), blk)], own.at[m, pl.ds(0, blk)], load_sem.at[i]).start()
    par_cp = pltpu.make_async_copy(par_hbm, par, load_sem.at[3])
    par_cp.start()
    acc_cp = pltpu.make_async_copy(acc_hbm, acc, load_sem.at[4])
    acc_cp.start()

    barrier = pltpu.get_barrier_semaphore()
    near = [place(d, c) for d in (X, Y, Z) for c in (core, 1 - core)] + [partner]
    for dev in near:
        pl.semaphore_signal(barrier, inc=1, device_id=(dev,), device_id_type=MESH)
    pl.semaphore_wait(barrier, len(near))

    all_bits = X + Y + Z
    pieces = [cut(s0 + FIRST, size - FIRST, PIECES) for s0, size in thirds]

    def exchange(m, start, size, i):
        send(grad_hbm.at[pl.ds(base(m, 1 - core) + start, size)],
             part.at[m, pl.ds(start, size)], 0, near_sem.at[i], partner)

    for t in range(3):
        s0, _ = thirds[t]
        for c, dst in ((core, recv), (1 - core, other)):
            send(grad_hbm.at[pl.ds(base(all_bits, c) + s0, FIRST)], dst.at[t, pl.ds(0, FIRST)],
                 1, far_sem.at[0], place(ORDERS[t][0], c))
    for p in range(PIECES):
        for t in range(3):
            exchange(all_bits, *pieces[t][p], p)
    for i in (1, 2):
        for m in waves[i]:
            exchange(m, 0, blk, PIECES - 1 + i)

    def fold(m, start, size):
        r = pl.ds(start, size)
        own[m, r] = own[m, r] + part[m, r]

    def unit(step, t):
        a, b, c = ORDERS[t]
        return (b + c, b, c, 0, c, 0, 0)[step]

    PHASE = (0, 0, 0, 0, 1, 1, 2)

    def push(step, t, start, size):
        dim = ORDERS[t][PHASE[step]]
        s0 = thirds[t][0]
        send(own.at[unit(step, t) ^ dim, pl.ds(start, size)],
             recv.at[3 * step + t, pl.ds(start - s0, size)], 1, far_sem.at[step], across[dim])

    load_waits = [len(w) * blk for w in waves]
    wait_rows(load_sem.at[0], load_waits[0])
    for p in range(PIECES):
        wait_rows(near_sem.at[p], sum(pieces[t][p][1] for t in range(3)))
        for t in range(3):
            fold(all_bits, *pieces[t][p])
            push(0, t, *pieces[t][p])
    wait_rows(load_sem.at[1], load_waits[1])
    wait_rows(near_sem.at[PIECES], load_waits[1])
    for step in (1, 2):
        for t in range(3):
            fold(unit(step, t) ^ ORDERS[t][0], *thirds[t])
            push(step, t, *thirds[t])
    wait_rows(load_sem.at[2], load_waits[2])
    wait_rows(near_sem.at[PIECES + 1], load_waits[2])
    for t in range(3):
        fold(unit(3, t) ^ ORDERS[t][0], *thirds[t])
        push(3, t, *thirds[t])
    for step in range(4):
        for t in range(3):
            fold(unit(step, t), *thirds[t])

    def early(k, src, lo, hi):
        for t in range(3):
            send(src.at[pl.ds(thirds[t][0] + lo, hi - lo)], raw.at[3 * t + k, pl.ds(lo, hi - lo)],
                 5, raw_sem, across[ORDERS[t][2]])

    par_cp.wait()
    acc_cp.wait()
    total = jnp.zeros((1, LANES), jnp.float32)
    for step in range(7):
        wait_rows(far_sem.at[step], blk if step else blk + 3 * FIRST)
        for t in range(3):
            m = unit(step, t)
            s0, size = thirds[t]
            if step == 0:
                r = pl.ds(0, FIRST)
                recv[t, r] = recv[t, r] + other[t, r]
            got = own[m, pl.ds(s0, size)] + recv[3 * step + t, pl.ds(0, size)]
            own[m, pl.ds(s0, size)] = got
            if step in (0, 1):
                push(4 + step, t, *thirds[t])
            if step == 4:
                push(6, t, *thirds[t])
            if step == 6:
                g = got * (1.0 / groups)
                total = total + jnp.sum(g * g, axis=0, keepdims=True)
        if step == 4:
            early(0, par, 0, AHEAD)
            early(1, acc, 0, AHEAD)

    slots[pl.ds(me, 1)] = total
    mine = slots.at[pl.ds(me, 1)]
    for m in (7, 3, 6, 5, 1, 2, 4):
        for c in (core, 1 - core):
            send(mine, mine, 2, nrm_sem, place(m, c))
    send(mine, mine, 2, nrm_sem, partner)
    early(2, own.at[0], 0, EARLY)
    early(0, par, AHEAD, EARLY)
    early(1, acc, AHEAD, EARLY)
    wait_rows(nrm_sem, groups - 1)
    square = jnp.sum(jnp.sum(slots[...], axis=0, keepdims=True), axis=1, keepdims=True)
    norm = jnp.sqrt(square)
    norm_ref[...] = jnp.broadcast_to(norm, (1, LANES))
    scale = jnp.minimum(1.0, clip_ref[...] / norm)
    rate = rate_ref[...]

    def rows(m, start, size, c=core):
        return full.at[pl.ds(base(m, c) + start, size)]

    def gather(m, t, j, rcv, start, size):
        send(rows(m, start, size), rows(m, start, size), 3, rcv, across[ORDERS[t][2 - j]])

    def forward(m, start, size, c=core):
        send(rows(m, start, size, c), rows(m, start, size, c), 4, near_sem.at[PIECES], partner)

    def update(w, a, total):
        h = total * (1.0 / groups) * scale
        a_new = a + h * h
        return a_new, w - rate * h / (jnp.sqrt(a_new) + EPS)

    heads = [cut(s0 + EARLY, size - EARLY, 3) + [(s0, EARLY)] for s0, size in thirds]
    for p in range(4):
        for t in range(3):
            start, size = heads[t][p]
            r = pl.ds(start, size)
            newa_ref[r], full[pl.ds(base(0, core) + start, size)] = update(par[r], acc[r], own[0, r])
            if p < 3:
                gather(0, t, 0, far_sem.at[0], start, size)
    for j in (1, 2):
        for t in range(3):
            gather(0, t, j, far_sem.at[j], *thirds[t])
    forward(0, 0, blk)
    wait_rows(raw_sem, 9 * EARLY)
    for t in range(3):
        r = pl.ds(0, EARLY)
        full[pl.ds(base(ORDERS[t][2], core) + thirds[t][0], EARLY)] = update(
            raw[3 * t, r], raw[3 * t + 1, r], raw[3 * t + 2, r])[1]

    tails = [cut(s0, size - BOTH, PIECES) for s0, size in thirds]
    ends = [(s0 + size - BOTH, BOTH) for s0, size in thirds]
    for step in range(6):
        wait_rows(far_sem.at[step], blk if step else blk - 3 * EARLY)
        for t in range(3):
            c, b, a = ORDERS[t]
            m = (a, b, c, a + b, a + c, b + c)[step]
            if step == 0:
                gather(m, t, 1, far_sem.at[3], *thirds[t])
            if step in (0, 1):
                gather(m, t, 2, far_sem.at[4 + step], *thirds[t])
            if step == 3:
                for p in range(PIECES):
                    r = rows(m, *tails[t][p])
                    send(r, r, 3, near_sem.at[p], place(ORDERS[t][0], 1 - core))
        if step == 3:
            last = [(rows(a + b, *ends[t]), c) for t, (c, b, a) in enumerate(ORDERS)]

            @pl.when(core == 0)
            def _():
                for r, c in last:
                    send(r, r, 3, nrm_sem, place(c, 0))

            for r, c in last:
                send(r, r, 3, near_sem.at[PIECES + 1], place(c, 1 - core))
        for t in range(3):
            c, b, a = ORDERS[t]
            forward((a, b, c, a + b, a + c, b + c)[step], *thirds[t])
    for p in range(PIECES):
        wait_rows(near_sem.at[p], sum(tails[t][p][1] for t in range(3)))
        for t in range(3):
            forward(all_bits, *tails[t][p], 1 - core)
    n_both = sum(size for _, size in ends)
    wait_rows(near_sem.at[PIECES + 1], n_both)

    @pl.when(core == 0)
    def _():
        for t in range(3):
            forward(all_bits, *ends[t], 1)
        wait_rows(nrm_sem, n_both)
        wait_rows(near_sem.at[PIECES], 8 * blk - n_both)
        wait_rows(send_sem.at[3], n_both)
        wait_rows(send_sem.at[4], n_both)

    @pl.when(core == 1)
    def _():
        wait_rows(near_sem.at[PIECES], 8 * blk)

    for kind, n in enumerate(
            (8 * blk - 3 * FIRST, 7 * blk + 3 * FIRST, groups - 1, 7 * blk - 3 * EARLY, 8 * blk - n_both, 9 * EARLY)):
        wait_rows(send_sem.at[kind], n)


def write_kernel(blk, full, newa, norm, newp_hbm, newa_hbm, copy_hbm, norm_hbm, buf, one, sems):
    me = lax.axis_index("dp")
    mine = full.at[pl.ds(me * blk, blk)]
    one[...] = norm[:, :1]
    out = [
        pltpu.make_async_copy(mine, newp_hbm, sems.at[0]),
        pltpu.make_async_copy(newa, newa_hbm, sems.at[1]),
        pltpu.make_async_copy(one, norm_hbm, sems.at[2]),
    ]
    for cp in out:
        cp.start()
    n = full.shape[0]
    edges = [n * i // TILES // 16 * 16 for i in range(TILES)] + [n]
    for i in range(TILES):
        r = pl.ds(edges[i], edges[i + 1] - edges[i])
        buf[r] = full[r].astype(jnp.bfloat16)
        pltpu.make_async_copy(buf.at[r], copy_hbm.at[r], sems.at[3]).start()
    pltpu.make_async_copy(buf, copy_hbm, sems.at[3]).wait()
    for cp in out:
        cp.wait()


def in_hbm(a):
    return pltpu.with_memory_space_constraint(a, pltpu.HBM)


def solution(mesh):
    groups = mesh.shape["dp"]

    def local_step(grad_row, param_blk, accum_blk, learn_rate, clip_max):
        n = grad_row.shape[1] // LANES
        blk = n // groups
        third = -(-blk // 24) * 8
        pad = -(-blk // 8) * 8
        f32 = jnp.float32
        vm = pl.BlockSpec(memory_space=pltpu.VMEM)
        sm = pl.BlockSpec(memory_space=pltpu.SMEM)
        hb = pl.BlockSpec(memory_space=pltpu.HBM)
        dma = pltpu.SemaphoreType.DMA
        full, newa, norm = pl.pallas_call(
            functools.partial(kernel, blk, third, groups),
            out_shape=(
                pltpu.VMEM((n, LANES), f32),
                pltpu.VMEM((blk, LANES), f32),
                pltpu.VMEM((1, LANES), f32),
            ),
            in_specs=[sm, sm, hb, hb, hb],
            out_specs=(vm, vm, vm),
            scratch_shapes=[
                pltpu.VMEM((8, pad, LANES), f32),
                pltpu.VMEM((8, pad, LANES), f32),
                pltpu.VMEM((21, third, LANES), f32),
                pltpu.VMEM((3, FIRST, LANES), f32),
                pltpu.VMEM((blk, LANES), f32),
                pltpu.VMEM((blk, LANES), f32),
                pltpu.VMEM((groups, LANES), f32),
                pltpu.VMEM((9, EARLY, LANES), f32),
                dma((5,)), dma((PIECES + 2,)), dma((7,)), dma, dma, dma((6,)),
            ],
            compiler_params=pltpu.CompilerParams(
                collective_id=0, has_side_effects=True, vmem_limit_bytes=40 * 1024 * 1024),
        )(learn_rate, clip_max, in_hbm(grad_row.reshape(n, LANES)),
          in_hbm(param_blk.reshape(blk, LANES)), in_hbm(accum_blk.reshape(blk, LANES)))
        newp, newa, copy, norm = pl.pallas_call(
            functools.partial(write_kernel, blk),
            out_shape=(
                jax.ShapeDtypeStruct((blk, LANES), f32),
                jax.ShapeDtypeStruct((blk, LANES), f32),
                jax.ShapeDtypeStruct((n, LANES), jnp.bfloat16),
                jax.ShapeDtypeStruct((1, 1), f32),
            ),
            in_specs=[vm, vm, vm],
            out_specs=(hb, hb, hb, hb),
            scratch_shapes=[pltpu.VMEM((n, LANES), jnp.bfloat16), pltpu.VMEM((1, 1), f32), dma((4,))],
            compiler_params=pltpu.CompilerParams(vmem_limit_bytes=12 * 1024 * 1024),
        )(full, newa, norm)
        return newp.reshape(-1), newa.reshape(-1), copy.reshape(-1), norm.reshape(())

    return jax.shard_map(local_step, mesh=mesh, in_specs=(P("dp", None), P("dp"), P("dp"), P(), P()), out_specs=(P("dp"), P("dp"), P(), P()), check_vma=False)
```

```python
import functools
import jax
import jax.numpy as jnp
from jax import lax
from jax.sharding import PartitionSpec as P
from jax.experimental import pallas as pl
from jax.experimental.pallas import tpu as pltpu

EPS = 1e-10
LANES = 128
X, Y, Z = 1, 2, 4
ORDERS = ((X, Y, Z), (Y, Z, X), (Z, X, Y))
MESH = pl.DeviceIdType.MESH
TILES = 12
PIECES = 6
AHEAD = 104
EARLY = 160
BOTH = 112
FIRST = 64


def cut(start, size, n):
    step = -(-size // (8 * n)) * 8
    return [(start + i * step, min(step, size - i * step)) for i in range(n)]


def kernel(
    blk, third, groups,
    rate_ref, clip_ref, grad_hbm, par_hbm, acc_hbm,
    full, newa_ref, norm_ref,
    own, part, recv, guest, other, par, acc, slots, raw,
    load_sem, near_sem, far_sem, nrm_sem, raw_sem, send_sem,
):
    me = lax.axis_index("dp")
    core = me % 2
    chip = me // 2
    x, y, z = chip % 2, (chip // 2) % 2, chip // 4
    partner = me + 1 - 2 * core
    across = {X: me + 2 - 4 * x, Y: me + 4 - 8 * y, Z: me + 8 - 16 * z}

    def place(m, c):
        xc = 1 - x if m & X else x
        yc = 1 - y if m & Y else y
        zc = 1 - z if m & Z else z
        return 2 * (4 * zc + 2 * yc + xc) + c

    def base(m, c):
        return blk * place(m, c)

    thirds = [(third * t, min(third, blk - third * t)) for t in range(3)]

    def send(src, dst, kind, rcv, dev):
        pltpu.make_async_remote_copy(
            src_ref=src, dst_ref=dst, send_sem=send_sem.at[kind], recv_sem=rcv,
            device_id=(dev,), device_id_type=MESH).start()

    def wait_rows(sem, n):
        ref = full.at[pl.ds(0, n)]
        pltpu.make_async_copy(ref, ref, sem).wait()

    waves = ((X + Y + Z,), (X + Y, Y + Z, Z + X), (X, Y, Z, 0))
    for i, wave in enumerate(waves):
        for m in wave:
            pltpu.make_async_copy(
                grad_hbm.at[pl.ds(base(m, core), blk)], own.at[m, pl.ds(0, blk)], load_sem.at[i]).start()
    par_cp = pltpu.make_async_copy(par_hbm, par, load_sem.at[3])
    par_cp.start()
    acc_cp = pltpu.make_async_copy(acc_hbm, acc, load_sem.at[4])
    acc_cp.start()

    barrier = pltpu.get_barrier_semaphore()
    near = (partner, across[X], across[Y], across[Z])
    for dev in near:
        pl.semaphore_signal(barrier, inc=1, device_id=(dev,), device_id_type=MESH)
    pl.semaphore_wait(barrier, len(near))

    all_bits = X + Y + Z
    pieces = [cut(s0 + FIRST, size - FIRST, PIECES) for s0, size in thirds]

    def exchange(m, start, size, i):
        send(grad_hbm.at[pl.ds(base(m, 1 - core) + start, size)],
             part.at[m, pl.ds(start, size)], 0, near_sem.at[i], partner)

    for t in range(3):
        s0, _ = thirds[t]
        for c, dst, i in ((core, recv, 0), (1 - core, guest, 7)):
            send(grad_hbm.at[pl.ds(base(all_bits, c) + s0, FIRST)], dst.at[t, pl.ds(0, FIRST)],
                 1, far_sem.at[i], across[ORDERS[t][0]])
    for p in range(PIECES):
        for t in range(3):
            exchange(all_bits, *pieces[t][p], p)
    for i in (1, 2):
        for m in waves[i]:
            exchange(m, 0, blk, PIECES - 1 + i)

    def fold(m, start, size):
        r = pl.ds(start, size)
        own[m, r] = own[m, r] + part[m, r]

    def unit(step, t):
        a, b, c = ORDERS[t]
        return (b + c, b, c, 0, c, 0, 0)[step]

    PHASE = (0, 0, 0, 0, 1, 1, 2)

    def push(step, t, start, size):
        dim = ORDERS[t][PHASE[step]]
        s0 = thirds[t][0]
        send(own.at[unit(step, t) ^ dim, pl.ds(start, size)],
             recv.at[3 * step + t, pl.ds(start - s0, size)], 1, far_sem.at[step], across[dim])

    load_waits = [len(w) * blk for w in waves]
    wait_rows(load_sem.at[0], load_waits[0])
    for p in range(PIECES):
        wait_rows(near_sem.at[p], sum(pieces[t][p][1] for t in range(3)))
        for t in range(3):
            fold(all_bits, *pieces[t][p])
            push(0, t, *pieces[t][p])
    wait_rows(load_sem.at[1], load_waits[1])
    wait_rows(near_sem.at[PIECES], load_waits[1])
    for step in (1, 2):
        for t in range(3):
            fold(unit(step, t) ^ ORDERS[t][0], *thirds[t])
            push(step, t, *thirds[t])
    wait_rows(load_sem.at[2], load_waits[2])
    wait_rows(near_sem.at[PIECES + 1], load_waits[2])
    for t in range(3):
        fold(unit(3, t) ^ ORDERS[t][0], *thirds[t])
        push(3, t, *thirds[t])
    wait_rows(far_sem.at[7], 3 * FIRST)
    send(guest, other, 0, near_sem.at[PIECES + 2], partner)
    for step in range(4):
        for t in range(3):
            fold(unit(step, t), *thirds[t])

    def early(k, src, lo, hi):
        for t in range(3):
            send(src.at[pl.ds(thirds[t][0] + lo, hi - lo)], raw.at[3 * t + k, pl.ds(lo, hi - lo)],
                 5, raw_sem, across[ORDERS[t][2]])

    par_cp.wait()
    acc_cp.wait()
    total = jnp.zeros((1, LANES), jnp.float32)
    for step in range(7):
        wait_rows(far_sem.at[step], blk)
        if step == 0:
            wait_rows(near_sem.at[PIECES + 2], 3 * FIRST)
        for t in range(3):
            m = unit(step, t)
            s0, size = thirds[t]
            if step == 0:
                r = pl.ds(0, FIRST)
                recv[t, r] = recv[t, r] + other[t, r]
            got = own[m, pl.ds(s0, size)] + recv[3 * step + t, pl.ds(0, size)]
            own[m, pl.ds(s0, size)] = got
            if step in (0, 1):
                push(4 + step, t, *thirds[t])
            if step == 4:
                push(6, t, *thirds[t])
            if step == 6:
                g = got * (1.0 / groups)
                total = total + jnp.sum(g * g, axis=0, keepdims=True)
        if step == 4:
            early(0, par, 0, AHEAD)
            early(1, acc, 0, AHEAD)

    slots[pl.ds(me, 1)] = total
    mine = slots.at[pl.ds(me, 1)]
    for m in (7, 3, 6, 5, 1, 2, 4):
        for c in (core, 1 - core):
            send(mine, mine, 2, nrm_sem, place(m, c))
    send(mine, mine, 2, nrm_sem, partner)
    early(2, own.at[0], 0, EARLY)
    early(0, par, AHEAD, EARLY)
    early(1, acc, AHEAD, EARLY)
    wait_rows(nrm_sem, groups - 1)
    square = jnp.sum(jnp.sum(slots[...], axis=0, keepdims=True), axis=1, keepdims=True)
    norm = jnp.sqrt(square)
    norm_ref[...] = jnp.broadcast_to(norm, (1, LANES))
    scale = jnp.minimum(1.0, clip_ref[...] / norm)
    rate = rate_ref[...]

    def rows(m, start, size, c=core):
        return full.at[pl.ds(base(m, c) + start, size)]

    def gather(m, t, j, rcv, start, size):
        send(rows(m, start, size), rows(m, start, size), 3, rcv, across[ORDERS[t][2 - j]])

    def forward(m, start, size, c=core):
        send(rows(m, start, size, c), rows(m, start, size, c), 4, near_sem.at[PIECES], partner)

    def update(w, a, total):
        h = total * (1.0 / groups) * scale
        a_new = a + h * h
        return a_new, w - rate * h / (jnp.sqrt(a_new) + EPS)

    heads = [cut(s0 + EARLY, size - EARLY, 3) + [(s0, EARLY)] for s0, size in thirds]
    for p in range(4):
        for t in range(3):
            start, size = heads[t][p]
            r = pl.ds(start, size)
            newa_ref[r], full[pl.ds(base(0, core) + start, size)] = update(par[r], acc[r], own[0, r])
            if p < 3:
                gather(0, t, 0, far_sem.at[0], start, size)
    for j in (1, 2):
        for t in range(3):
            gather(0, t, j, far_sem.at[j], *thirds[t])
    forward(0, 0, blk)
    wait_rows(raw_sem, 9 * EARLY)
    for t in range(3):
        r = pl.ds(0, EARLY)
        full[pl.ds(base(ORDERS[t][2], core) + thirds[t][0], EARLY)] = update(
            raw[3 * t, r], raw[3 * t + 1, r], raw[3 * t + 2, r])[1]

    tails = [cut(s0, size - BOTH, PIECES) for s0, size in thirds]
    ends = [(s0 + size - BOTH, BOTH) for s0, size in thirds]
    for step in range(6):
        wait_rows(far_sem.at[step], blk if step else blk - 3 * EARLY)
        for t in range(3):
            c, b, a = ORDERS[t]
            m = (a, b, c, a + b, a + c, b + c)[step]
            if step == 0:
                gather(m, t, 1, far_sem.at[3], *thirds[t])
            if step in (0, 1):
                gather(m, t, 2, far_sem.at[4 + step], *thirds[t])
            if step == 3:
                for p in range(PIECES):
                    r = rows(m, *tails[t][p])
                    send(r, r, 3, near_sem.at[p], place(ORDERS[t][0], 1 - core))
        if step == 3:
            last = [(rows(a + b, *ends[t]), c) for t, (c, b, a) in enumerate(ORDERS)]

            @pl.when(core == 0)
            def _():
                for r, c in last:
                    send(r, r, 3, nrm_sem, place(c, 0))

            for r, c in last:
                send(r, r, 3, near_sem.at[PIECES + 1], place(c, 1 - core))
        for t in range(3):
            c, b, a = ORDERS[t]
            forward((a, b, c, a + b, a + c, b + c)[step], *thirds[t])
    for p in range(PIECES):
        wait_rows(near_sem.at[p], sum(tails[t][p][1] for t in range(3)))
        for t in range(3):
            forward(all_bits, *tails[t][p], 1 - core)
    n_both = sum(size for _, size in ends)
    wait_rows(near_sem.at[PIECES + 1], n_both)

    @pl.when(core == 0)
    def _():
        for t in range(3):
            forward(all_bits, *ends[t], 1)
        wait_rows(nrm_sem, n_both)
        wait_rows(near_sem.at[PIECES], 8 * blk - n_both)
        wait_rows(send_sem.at[3], n_both)
        wait_rows(send_sem.at[4], n_both)

    @pl.when(core == 1)
    def _():
        wait_rows(near_sem.at[PIECES], 8 * blk)

    for kind, n in enumerate(
            (8 * blk, 7 * blk + 3 * FIRST, groups - 1, 7 * blk - 3 * EARLY, 8 * blk - n_both, 9 * EARLY)):
        wait_rows(send_sem.at[kind], n)


def write_kernel(blk, full, newa, norm, newp_hbm, newa_hbm, copy_hbm, norm_hbm, buf, one, sems):
    me = lax.axis_index("dp")
    mine = full.at[pl.ds(me * blk, blk)]
    one[...] = norm[:, :1]
    out = [
        pltpu.make_async_copy(mine, newp_hbm, sems.at[0]),
        pltpu.make_async_copy(newa, newa_hbm, sems.at[1]),
        pltpu.make_async_copy(one, norm_hbm, sems.at[2]),
    ]
    for cp in out:
        cp.start()
    n = full.shape[0]
    edges = [n * i // TILES // 16 * 16 for i in range(TILES)] + [n]
    for i in range(TILES):
        r = pl.ds(edges[i], edges[i + 1] - edges[i])
        buf[r] = full[r].astype(jnp.bfloat16)
        pltpu.make_async_copy(buf.at[r], copy_hbm.at[r], sems.at[3]).start()
    pltpu.make_async_copy(buf, copy_hbm, sems.at[3]).wait()
    for cp in out:
        cp.wait()


def in_hbm(a):
    return pltpu.with_memory_space_constraint(a, pltpu.HBM)


def solution(mesh):
    groups = mesh.shape["dp"]

    def local_step(grad_row, param_blk, accum_blk, learn_rate, clip_max):
        n = grad_row.shape[1] // LANES
        blk = n // groups
        third = -(-blk // 24) * 8
        pad = -(-blk // 8) * 8
        f32 = jnp.float32
        vm = pl.BlockSpec(memory_space=pltpu.VMEM)
        sm = pl.BlockSpec(memory_space=pltpu.SMEM)
        hb = pl.BlockSpec(memory_space=pltpu.HBM)
        dma = pltpu.SemaphoreType.DMA
        full, newa, norm = pl.pallas_call(
            functools.partial(kernel, blk, third, groups),
            out_shape=(
                pltpu.VMEM((n, LANES), f32),
                pltpu.VMEM((blk, LANES), f32),
                pltpu.VMEM((1, LANES), f32),
            ),
            in_specs=[sm, sm, hb, hb, hb],
            out_specs=(vm, vm, vm),
            scratch_shapes=[
                pltpu.VMEM((8, pad, LANES), f32),
                pltpu.VMEM((8, pad, LANES), f32),
                pltpu.VMEM((21, third, LANES), f32),
                pltpu.VMEM((3, FIRST, LANES), f32),
                pltpu.VMEM((3, FIRST, LANES), f32),
                pltpu.VMEM((blk, LANES), f32),
                pltpu.VMEM((blk, LANES), f32),
                pltpu.VMEM((groups, LANES), f32),
                pltpu.VMEM((9, EARLY, LANES), f32),
                dma((5,)), dma((PIECES + 3,)), dma((8,)), dma, dma, dma((6,)),
            ],
            compiler_params=pltpu.CompilerParams(
                collective_id=0, has_side_effects=True, vmem_limit_bytes=40 * 1024 * 1024),
        )(learn_rate, clip_max, in_hbm(grad_row.reshape(n, LANES)),
          in_hbm(param_blk.reshape(blk, LANES)), in_hbm(accum_blk.reshape(blk, LANES)))
        newp, newa, copy, norm = pl.pallas_call(
            functools.partial(write_kernel, blk),
            out_shape=(
                jax.ShapeDtypeStruct((blk, LANES), f32),
                jax.ShapeDtypeStruct((blk, LANES), f32),
                jax.ShapeDtypeStruct((n, LANES), jnp.bfloat16),
                jax.ShapeDtypeStruct((1, 1), f32),
            ),
            in_specs=[vm, vm, vm],
            out_specs=(hb, hb, hb, hb),
            scratch_shapes=[pltpu.VMEM((n, LANES), jnp.bfloat16), pltpu.VMEM((1, 1), f32), dma((4,))],
            compiler_params=pltpu.CompilerParams(vmem_limit_bytes=12 * 1024 * 1024),
        )(full, newa, norm)
        return newp.reshape(-1), newa.reshape(-1), copy.reshape(-1), norm.reshape(())

    return jax.shard_map(local_step, mesh=mesh, in_specs=(P("dp", None), P("dp"), P("dp"), P(), P()), out_specs=(P("dp"), P("dp"), P(), P()), check_vma=False)
```

```python
import functools
import jax
import jax.numpy as jnp
from jax import lax
from jax.sharding import PartitionSpec as P
from jax.experimental import pallas as pl
from jax.experimental.pallas import tpu as pltpu

EPS = 1e-10
LANES = 128
X, Y, Z = 1, 2, 4
ORDERS = ((X, Y, Z), (Y, Z, X), (Z, X, Y))
MESH = pl.DeviceIdType.MESH
TILES = 12
PIECES = 6
AHEAD = 104
EARLY = 160
BOTH = 120
FIRST = 64


def cut(start, size, n):
    step = -(-size // (8 * n)) * 8
    return [(start + i * step, min(step, size - i * step)) for i in range(n)]


def kernel(
    blk, third, groups,
    rate_ref, clip_ref, grad_hbm, par_hbm, acc_hbm,
    full, newa_ref, norm_ref,
    own, part, recv, guest, other, par, acc, slots, raw,
    load_sem, near_sem, far_sem, nrm_sem, raw_sem, send_sem,
):
    me = lax.axis_index("dp")
    core = me % 2
    chip = me // 2
    x, y, z = chip % 2, (chip // 2) % 2, chip // 4
    partner = me + 1 - 2 * core
    across = {X: me + 2 - 4 * x, Y: me + 4 - 8 * y, Z: me + 8 - 16 * z}

    def place(m, c):
        xc = 1 - x if m & X else x
        yc = 1 - y if m & Y else y
        zc = 1 - z if m & Z else z
        return 2 * (4 * zc + 2 * yc + xc) + c

    def base(m, c):
        return blk * place(m, c)

    thirds = [(third * t, min(third, blk - third * t)) for t in range(3)]

    def send(src, dst, rcv, dev):
        pltpu.make_async_remote_copy(
            src_ref=src, dst_ref=dst, send_sem=send_sem, recv_sem=rcv,
            device_id=(dev,), device_id_type=MESH).start()

    def wait_rows(sem, n):
        ref = full.at[pl.ds(0, n)]
        pltpu.make_async_copy(ref, ref, sem).wait()

    barrier = pltpu.get_barrier_semaphore()
    near = (across[X], across[Y], across[Z], partner)
    for dev in near:
        pl.semaphore_signal(barrier, inc=1, device_id=(dev,), device_id_type=MESH)

    waves = ((X + Y + Z,), (X + Y, Y + Z, Z + X), (X, Y, Z, 0))
    for i, wave in enumerate(waves):
        for m in wave:
            pltpu.make_async_copy(
                grad_hbm.at[pl.ds(base(m, core), blk)], own.at[m, pl.ds(0, blk)], load_sem.at[i]).start()
    pltpu.make_async_copy(par_hbm, par, load_sem.at[2]).start()
    pltpu.make_async_copy(acc_hbm, acc, load_sem.at[2]).start()

    pl.semaphore_wait(barrier, len(near))

    all_bits = X + Y + Z
    pieces = [cut(s0 + FIRST, size - FIRST, PIECES) for s0, size in thirds]

    def exchange(m, start, size, i):
        send(grad_hbm.at[pl.ds(base(m, 1 - core) + start, size)],
             part.at[m, pl.ds(start, size)], near_sem.at[i], partner)

    for t in range(3):
        s0, _ = thirds[t]
        for c, dst, i in ((core, recv, 0), (1 - core, guest, 7)):
            send(grad_hbm.at[pl.ds(base(all_bits, c) + s0, FIRST)], dst.at[t, pl.ds(0, FIRST)],
                 far_sem.at[i], across[ORDERS[t][0]])
    for p in range(PIECES):
        for t in range(3):
            exchange(all_bits, *pieces[t][p], p)
    for i in (1, 2):
        for m in waves[i]:
            exchange(m, 0, blk, PIECES - 1 + i)

    def fold(m, start, size):
        r = pl.ds(start, size)
        own[m, r] = own[m, r] + part[m, r]

    def unit(step, t):
        a, b, c = ORDERS[t]
        return (b + c, b, c, 0, c, 0, 0)[step]

    PHASE = (0, 0, 0, 0, 1, 1, 2)

    def push(step, t, start, size):
        dim = ORDERS[t][PHASE[step]]
        s0 = thirds[t][0]
        send(own.at[unit(step, t) ^ dim, pl.ds(start, size)],
             recv.at[3 * step + t, pl.ds(start - s0, size)], far_sem.at[step], across[dim])

    load_waits = [len(w) * blk for w in waves]
    wait_rows(load_sem.at[0], load_waits[0])
    for p in range(PIECES):
        wait_rows(near_sem.at[p], sum(pieces[t][p][1] for t in range(3)))
        for t in range(3):
            fold(all_bits, *pieces[t][p])
            push(0, t, *pieces[t][p])
    wait_rows(load_sem.at[1], load_waits[1])
    wait_rows(near_sem.at[PIECES], load_waits[1])
    for step in (1, 2):
        for t in range(3):
            fold(unit(step, t) ^ ORDERS[t][0], *thirds[t])
            push(step, t, *thirds[t])
    wait_rows(load_sem.at[2], load_waits[2] + 2 * blk)
    wait_rows(near_sem.at[PIECES + 1], load_waits[2])
    for t in range(3):
        fold(unit(3, t) ^ ORDERS[t][0], *thirds[t])
        push(3, t, *thirds[t])
    wait_rows(far_sem.at[7], 3 * FIRST)
    send(guest, other, near_sem.at[PIECES + 2], partner)
    for step in range(4):
        for t in range(3):
            fold(unit(step, t), *thirds[t])

    def early(k, src, lo, hi):
        for t in range(3):
            send(src.at[pl.ds(thirds[t][0] + lo, hi - lo)], raw.at[3 * t + k, pl.ds(lo, hi - lo)],
                 raw_sem, across[ORDERS[t][2]])

    total = jnp.zeros((1, LANES), jnp.float32)
    for step in range(7):
        wait_rows(far_sem.at[step], blk)
        if step == 0:
            wait_rows(near_sem.at[PIECES + 2], 3 * FIRST)
        for t in range(3):
            m = unit(step, t)
            s0, size = thirds[t]
            if step == 0:
                r = pl.ds(0, FIRST)
                recv[t, r] = recv[t, r] + other[t, r]
            got = own[m, pl.ds(s0, size)] + recv[3 * step + t, pl.ds(0, size)]
            own[m, pl.ds(s0, size)] = got
            if step in (0, 1):
                push(4 + step, t, *thirds[t])
            if step == 4:
                push(6, t, *thirds[t])
            if step == 6:
                g = got * (1.0 / groups)
                total = total + jnp.sum(g * g, axis=0, keepdims=True)
        if step == 4:
            early(0, par, 0, AHEAD)
            early(1, acc, 0, AHEAD)

    slots[pl.ds(me, 1)] = total
    mine = slots.at[pl.ds(me, 1)]
    for m in (7, 3, 6, 5, 1, 2, 4):
        for c in (core, 1 - core):
            send(mine, mine, nrm_sem, place(m, c))
    send(mine, mine, nrm_sem, partner)
    early(2, own.at[0], 0, EARLY)
    early(0, par, AHEAD, EARLY)
    early(1, acc, AHEAD, EARLY)
    wait_rows(nrm_sem, groups - 1)
    square = jnp.sum(jnp.sum(slots[...], axis=0, keepdims=True), axis=1, keepdims=True)
    norm = jnp.sqrt(square)
    norm_ref[...] = jnp.broadcast_to(norm, (1, LANES))
    scale = jnp.minimum(1.0, clip_ref[...] / norm)
    rate = rate_ref[...]

    def rows(m, start, size, c=core):
        return full.at[pl.ds(base(m, c) + start, size)]

    def gather(m, t, j, rcv, start, size):
        send(rows(m, start, size), rows(m, start, size), rcv, across[ORDERS[t][2 - j]])

    def forward(m, start, size, c=core):
        send(rows(m, start, size, c), rows(m, start, size, c), near_sem.at[PIECES], partner)

    def update(w, a, total):
        h = total * (1.0 / groups) * scale
        a_new = a + h * h
        return a_new, w - rate * h / (jnp.sqrt(a_new) + EPS)

    heads = [cut(s0 + EARLY, size - EARLY, 3) + [(s0, EARLY)] for s0, size in thirds]
    for p in range(4):
        for t in range(3):
            start, size = heads[t][p]
            r = pl.ds(start, size)
            newa_ref[r], full[pl.ds(base(0, core) + start, size)] = update(par[r], acc[r], own[0, r])
            if p < 3:
                gather(0, t, 0, far_sem.at[0], start, size)
    for j in (1, 2):
        for t in range(3):
            gather(0, t, j, far_sem.at[j], *thirds[t])
    forward(0, 0, blk)
    wait_rows(raw_sem, 9 * EARLY)
    for t in range(3):
        r = pl.ds(0, EARLY)
        full[pl.ds(base(ORDERS[t][2], core) + thirds[t][0], EARLY)] = update(
            raw[3 * t, r], raw[3 * t + 1, r], raw[3 * t + 2, r])[1]

    tails = [cut(s0, size - BOTH, PIECES) for s0, size in thirds]
    ends = [(s0 + size - BOTH, BOTH) for s0, size in thirds]
    for step in range(6):
        wait_rows(far_sem.at[step], blk if step else blk - 3 * EARLY)
        for t in range(3):
            c, b, a = ORDERS[t]
            m = (a, b, c, a + b, a + c, b + c)[step]
            if step == 0:
                gather(m, t, 1, far_sem.at[3], *thirds[t])
            if step in (0, 1):
                gather(m, t, 2, far_sem.at[4 + step], *thirds[t])
            if step == 3:
                for p in range(PIECES):
                    r = rows(m, *tails[t][p])
                    send(r, r, near_sem.at[p], place(ORDERS[t][0], 1 - core))
        if step == 3:
            last = [(rows(a + b, *ends[t]), c) for t, (c, b, a) in enumerate(ORDERS)]

            @pl.when(core == 0)
            def _():
                for r, c in last:
                    send(r, r, nrm_sem, place(c, 0))

            for r, c in last:
                send(r, r, near_sem.at[PIECES + 1], place(c, 1 - core))
        for t in range(3):
            c, b, a = ORDERS[t]
            forward((a, b, c, a + b, a + c, b + c)[step], *thirds[t])
    for p in range(PIECES):
        wait_rows(near_sem.at[p], sum(tails[t][p][1] for t in range(3)))
        for t in range(3):
            forward(all_bits, *tails[t][p], 1 - core)
    n_both = sum(size for _, size in ends)
    wait_rows(near_sem.at[PIECES + 1], n_both)

    @pl.when(core == 0)
    def _():
        for t in range(3):
            forward(all_bits, *ends[t], 1)
        wait_rows(nrm_sem, n_both)
        wait_rows(near_sem.at[PIECES], 8 * blk - n_both)
        wait_rows(send_sem, 2 * n_both)

    @pl.when(core == 1)
    def _():
        wait_rows(near_sem.at[PIECES], 8 * blk)

    for n in (8 * blk, 7 * blk + 3 * FIRST, groups - 1, 7 * blk - 3 * EARLY, 8 * blk - n_both, 9 * EARLY):
        wait_rows(send_sem, n)


def write_kernel(blk, full, newa, norm, newp_hbm, newa_hbm, copy_hbm, norm_hbm, buf, one, sems):
    me = lax.axis_index("dp")
    mine = full.at[pl.ds(me * blk, blk)]
    one[...] = norm[:, :1]
    out = [
        pltpu.make_async_copy(mine, newp_hbm, sems.at[0]),
        pltpu.make_async_copy(newa, newa_hbm, sems.at[1]),
        pltpu.make_async_copy(one, norm_hbm, sems.at[2]),
    ]
    for cp in out:
        cp.start()
    n = full.shape[0]
    edges = [n * i // TILES // 16 * 16 for i in range(TILES)] + [n]
    for i in range(TILES):
        r = pl.ds(edges[i], edges[i + 1] - edges[i])
        buf[r] = full[r].astype(jnp.bfloat16)
        pltpu.make_async_copy(buf.at[r], copy_hbm.at[r], sems.at[3]).start()
    pltpu.make_async_copy(buf, copy_hbm, sems.at[3]).wait()
    for cp in out:
        cp.wait()


def in_hbm(a):
    return pltpu.with_memory_space_constraint(a, pltpu.HBM)


def solution(mesh):
    groups = mesh.shape["dp"]

    def local_step(grad_row, param_blk, accum_blk, learn_rate, clip_max):
        n = grad_row.shape[1] // LANES
        blk = n // groups
        third = -(-blk // 24) * 8
        pad = -(-blk // 8) * 8
        f32 = jnp.float32
        vm = pl.BlockSpec(memory_space=pltpu.VMEM)
        sm = pl.BlockSpec(memory_space=pltpu.SMEM)
        hb = pl.BlockSpec(memory_space=pltpu.HBM)
        dma = pltpu.SemaphoreType.DMA
        full, newa, norm = pl.pallas_call(
            functools.partial(kernel, blk, third, groups),
            out_shape=(
                pltpu.VMEM((n, LANES), f32),
                pltpu.VMEM((blk, LANES), f32),
                pltpu.VMEM((1, LANES), f32),
            ),
            in_specs=[sm, sm, hb, hb, hb],
            out_specs=(vm, vm, vm),
            scratch_shapes=[
                pltpu.VMEM((8, pad, LANES), f32),
                pltpu.VMEM((8, pad, LANES), f32),
                pltpu.VMEM((21, third, LANES), f32),
                pltpu.VMEM((3, FIRST, LANES), f32),
                pltpu.VMEM((3, FIRST, LANES), f32),
                pltpu.VMEM((blk, LANES), f32),
                pltpu.VMEM((blk, LANES), f32),
                pltpu.VMEM((groups, LANES), f32),
                pltpu.VMEM((9, EARLY, LANES), f32),
                dma((3,)), dma((PIECES + 3,)), dma((8,)), dma, dma, dma,
            ],
            compiler_params=pltpu.CompilerParams(
                collective_id=0, has_side_effects=True, vmem_limit_bytes=40 * 1024 * 1024),
        )(learn_rate, clip_max, in_hbm(grad_row.reshape(n, LANES)),
          in_hbm(param_blk.reshape(blk, LANES)), in_hbm(accum_blk.reshape(blk, LANES)))
        newp, newa, copy, norm = pl.pallas_call(
            functools.partial(write_kernel, blk),
            out_shape=(
                jax.ShapeDtypeStruct((blk, LANES), f32),
                jax.ShapeDtypeStruct((blk, LANES), f32),
                jax.ShapeDtypeStruct((n, LANES), jnp.bfloat16),
                jax.ShapeDtypeStruct((1, 1), f32),
            ),
            in_specs=[vm, vm, vm],
            out_specs=(hb, hb, hb, hb),
            scratch_shapes=[pltpu.VMEM((n, LANES), jnp.bfloat16), pltpu.VMEM((1, 1), f32), dma((4,))],
            compiler_params=pltpu.CompilerParams(vmem_limit_bytes=12 * 1024 * 1024),
        )(full, newa, norm)
        return newp.reshape(-1), newa.reshape(-1), copy.reshape(-1), norm.reshape(())

    return jax.shard_map(local_step, mesh=mesh, in_specs=(P("dp", None), P("dp"), P("dp"), P(), P()), out_specs=(P("dp"), P("dp"), P(), P()), check_vma=False)
```

```python
import functools
import jax
import jax.numpy as jnp
from jax import lax
from jax.sharding import PartitionSpec as P
from jax.experimental import pallas as pl
from jax.experimental.pallas import tpu as pltpu

EPS = 1e-10
LANES = 128
X, Y, Z = 1, 2, 4
ORDERS = ((X, Y, Z), (Y, Z, X), (Z, X, Y))
MESH = pl.DeviceIdType.MESH
TILES = 20
PIECES = 6
AHEAD = 104
EARLY = 160
BOTH = 120
FIRST = 64


def cut(start, size, n):
    step = -(-size // (8 * n)) * 8
    return [(start + i * step, min(step, size - i * step)) for i in range(n)]


def kernel(
    blk, third, groups,
    rate_ref, clip_ref, grad_hbm, par_hbm, acc_hbm,
    full, newa_ref, norm_ref,
    own, part, recv, guest, other, par, acc, slots, raw,
    load_sem, near_sem, far_sem, nrm_sem, raw_sem, send_sem,
):
    me = lax.axis_index("dp")
    core = me % 2
    chip = me // 2
    x, y, z = chip % 2, (chip // 2) % 2, chip // 4
    partner = me + 1 - 2 * core
    across = {X: me + 2 - 4 * x, Y: me + 4 - 8 * y, Z: me + 8 - 16 * z}

    def place(m, c):
        xc = 1 - x if m & X else x
        yc = 1 - y if m & Y else y
        zc = 1 - z if m & Z else z
        return 2 * (4 * zc + 2 * yc + xc) + c

    def base(m, c):
        return blk * place(m, c)

    thirds = [(third * t, min(third, blk - third * t)) for t in range(3)]

    def send(src, dst, rcv, dev):
        pltpu.make_async_remote_copy(
            src_ref=src, dst_ref=dst, send_sem=send_sem, recv_sem=rcv,
            device_id=(dev,), device_id_type=MESH).start()

    def wait_rows(sem, n):
        ref = full.at[pl.ds(0, n)]
        pltpu.make_async_copy(ref, ref, sem).wait()

    barrier = pltpu.get_barrier_semaphore()
    near = (across[X], across[Y], across[Z], partner)
    for dev in near:
        pl.semaphore_signal(barrier, inc=1, device_id=(dev,), device_id_type=MESH)

    waves = ((X + Y + Z,), (X + Y, Y + Z, Z + X), (X, Y, Z, 0))
    for i, wave in enumerate(waves):
        for m in wave:
            pltpu.make_async_copy(
                grad_hbm.at[pl.ds(base(m, core), blk)], own.at[m, pl.ds(0, blk)], load_sem.at[i]).start()
    pltpu.make_async_copy(par_hbm, par, load_sem.at[2]).start()
    pltpu.make_async_copy(acc_hbm, acc, load_sem.at[2]).start()

    pl.semaphore_wait(barrier, len(near))

    all_bits = X + Y + Z
    pieces = [cut(s0 + FIRST, size - FIRST, PIECES) for s0, size in thirds]

    def exchange(m, start, size, i):
        send(grad_hbm.at[pl.ds(base(m, 1 - core) + start, size)],
             part.at[m, pl.ds(start, size)], near_sem.at[i], partner)

    for t in range(3):
        s0, _ = thirds[t]
        for c, dst, i in ((core, recv, 0), (1 - core, guest, 7)):
            send(grad_hbm.at[pl.ds(base(all_bits, c) + s0, FIRST)], dst.at[t, pl.ds(0, FIRST)],
                 far_sem.at[i], across[ORDERS[t][0]])
    for p in range(PIECES):
        for t in range(3):
            exchange(all_bits, *pieces[t][p], p)
    for i in (1, 2):
        for m in waves[i]:
            exchange(m, 0, blk, PIECES - 1 + i)

    def fold(m, start, size):
        r = pl.ds(start, size)
        own[m, r] = own[m, r] + part[m, r]

    def unit(step, t):
        a, b, c = ORDERS[t]
        return (b + c, b, c, 0, c, 0, 0)[step]

    PHASE = (0, 0, 0, 0, 1, 1, 2)

    def push(step, t, start, size):
        dim = ORDERS[t][PHASE[step]]
        s0 = thirds[t][0]
        send(own.at[unit(step, t) ^ dim, pl.ds(start, size)],
             recv.at[3 * step + t, pl.ds(start - s0, size)], far_sem.at[step], across[dim])

    load_waits = [len(w) * blk for w in waves]
    wait_rows(load_sem.at[0], load_waits[0])
    for p in range(PIECES):
        wait_rows(near_sem.at[p], sum(pieces[t][p][1] for t in range(3)))
        for t in range(3):
            fold(all_bits, *pieces[t][p])
            push(0, t, *pieces[t][p])
    wait_rows(load_sem.at[1], load_waits[1])
    wait_rows(near_sem.at[PIECES], load_waits[1])
    for step in (1, 2):
        for t in range(3):
            fold(unit(step, t) ^ ORDERS[t][0], *thirds[t])
            push(step, t, *thirds[t])
    wait_rows(load_sem.at[2], load_waits[2] + 2 * blk)
    wait_rows(near_sem.at[PIECES + 1], load_waits[2])
    for t in range(3):
        fold(unit(3, t) ^ ORDERS[t][0], *thirds[t])
        push(3, t, *thirds[t])
    wait_rows(far_sem.at[7], 3 * FIRST)
    send(guest, other, near_sem.at[PIECES + 2], partner)
    for step in range(4):
        for t in range(3):
            fold(unit(step, t), *thirds[t])

    def early(k, src, lo, hi):
        for t in range(3):
            send(src.at[pl.ds(thirds[t][0] + lo, hi - lo)], raw.at[3 * t + k, pl.ds(lo, hi - lo)],
                 raw_sem, across[ORDERS[t][2]])

    total = jnp.zeros((1, LANES), jnp.float32)
    for step in range(7):
        wait_rows(far_sem.at[step], blk)
        if step == 0:
            wait_rows(near_sem.at[PIECES + 2], 3 * FIRST)
        for t in range(3):
            m = unit(step, t)
            s0, size = thirds[t]
            if step == 0:
                r = pl.ds(0, FIRST)
                recv[t, r] = recv[t, r] + other[t, r]
            got = own[m, pl.ds(s0, size)] + recv[3 * step + t, pl.ds(0, size)]
            own[m, pl.ds(s0, size)] = got
            if step in (0, 1):
                push(4 + step, t, *thirds[t])
            if step == 4:
                push(6, t, *thirds[t])
            if step == 6:
                g = got * (1.0 / groups)
                total = total + jnp.sum(g * g, axis=0, keepdims=True)
        if step == 4:
            early(0, par, 0, AHEAD)
            early(1, acc, 0, AHEAD)

    slots[pl.ds(me, 1)] = total
    mine = slots.at[pl.ds(me, 1)]
    for m in (7, 3, 6, 5, 1, 2, 4):
        for c in (1 - core, core):
            send(mine, mine, nrm_sem, place(m, c))
    send(mine, mine, nrm_sem, partner)
    early(2, own.at[0], 0, EARLY)
    early(0, par, AHEAD, EARLY)
    early(1, acc, AHEAD, EARLY)
    wait_rows(nrm_sem, groups - 1)
    square = jnp.sum(jnp.sum(slots[...], axis=0, keepdims=True), axis=1, keepdims=True)
    norm = jnp.sqrt(square)
    norm_ref[...] = jnp.broadcast_to(norm, (1, LANES))
    scale = jnp.minimum(1.0, clip_ref[...] / norm)
    rate = rate_ref[...]

    def rows(m, start, size, c=core):
        return full.at[pl.ds(base(m, c) + start, size)]

    def gather(m, t, j, rcv, start, size):
        send(rows(m, start, size), rows(m, start, size), rcv, across[ORDERS[t][2 - j]])

    def forward(m, start, size, c=core):
        send(rows(m, start, size, c), rows(m, start, size, c), near_sem.at[PIECES], partner)

    def update(w, a, total):
        h = total * (1.0 / groups) * scale
        a_new = a + h * h
        return a_new, w - rate * h / (jnp.sqrt(a_new) + EPS)

    heads = [cut(s0 + EARLY, size - EARLY, 4) + [(s0, EARLY)] for s0, size in thirds]
    for p in range(5):
        for t in range(3):
            start, size = heads[t][p]
            r = pl.ds(start, size)
            newa_ref[r], full[pl.ds(base(0, core) + start, size)] = update(par[r], acc[r], own[0, r])
            if p < 4:
                gather(0, t, 0, far_sem.at[0], start, size)
    for j in (1, 2):
        for t in range(3):
            gather(0, t, j, far_sem.at[j], *thirds[t])
    forward(0, 0, blk)
    wait_rows(raw_sem, 9 * EARLY)
    for t in range(3):
        r = pl.ds(0, EARLY)
        full[pl.ds(base(ORDERS[t][2], core) + thirds[t][0], EARLY)] = update(
            raw[3 * t, r], raw[3 * t + 1, r], raw[3 * t + 2, r])[1]

    tails = [cut(s0, size - BOTH, PIECES) for s0, size in thirds]
    ends = [(s0 + size - BOTH, BOTH) for s0, size in thirds]
    for step in range(6):
        wait_rows(far_sem.at[step], blk if step else blk - 3 * EARLY)
        for t in range(3):
            c, b, a = ORDERS[t]
            m = (a, b, c, a + b, a + c, b + c)[step]
            if step == 0:
                gather(m, t, 1, far_sem.at[3], *thirds[t])
            if step in (0, 1):
                gather(m, t, 2, far_sem.at[4 + step], *thirds[t])
            if step == 3:
                for p in range(PIECES):
                    r = rows(m, *tails[t][p])
                    send(r, r, near_sem.at[p], place(ORDERS[t][0], 1 - core))
        if step == 3:
            last = [(rows(a + b, *ends[t]), c) for t, (c, b, a) in enumerate(ORDERS)]

            @pl.when(core == 0)
            def _():
                for r, c in last:
                    send(r, r, nrm_sem, place(c, 0))

            for r, c in last:
                send(r, r, near_sem.at[PIECES + 1], place(c, 1 - core))
        for t in range(3):
            c, b, a = ORDERS[t]
            forward((a, b, c, a + b, a + c, b + c)[step], *thirds[t])
    for p in range(PIECES):
        wait_rows(near_sem.at[p], sum(tails[t][p][1] for t in range(3)))
        for t in range(3):
            forward(all_bits, *tails[t][p], 1 - core)
    n_both = sum(size for _, size in ends)
    wait_rows(near_sem.at[PIECES + 1], n_both)

    @pl.when(core == 0)
    def _():
        for t in range(3):
            forward(all_bits, *ends[t], 1)
        wait_rows(nrm_sem, n_both)
        wait_rows(near_sem.at[PIECES], 8 * blk - n_both)
        wait_rows(send_sem, 2 * n_both)

    @pl.when(core == 1)
    def _():
        wait_rows(near_sem.at[PIECES], 8 * blk)

    for n in (8 * blk, 7 * blk + 3 * FIRST, groups - 1, 7 * blk - 3 * EARLY, 8 * blk - n_both, 9 * EARLY):
        wait_rows(send_sem, n)


def write_kernel(blk, full, newa, norm, newp_hbm, newa_hbm, copy_hbm, norm_hbm, buf, one, sems):
    me = lax.axis_index("dp")
    mine = full.at[pl.ds(me * blk, blk)]
    one[...] = norm[:, :1]
    out = [
        pltpu.make_async_copy(mine, newp_hbm, sems.at[0]),
        pltpu.make_async_copy(newa, newa_hbm, sems.at[1]),
        pltpu.make_async_copy(one, norm_hbm, sems.at[2]),
    ]
    for cp in out:
        cp.start()
    n = full.shape[0]
    edges = [n * i // TILES // 16 * 16 for i in range(TILES)] + [n]
    for i in range(TILES):
        r = pl.ds(edges[i], edges[i + 1] - edges[i])
        buf[r] = full[r].astype(jnp.bfloat16)
        pltpu.make_async_copy(buf.at[r], copy_hbm.at[r], sems.at[3]).start()
    pltpu.make_async_copy(buf, copy_hbm, sems.at[3]).wait()
    for cp in out:
        cp.wait()


def in_hbm(a):
    return pltpu.with_memory_space_constraint(a, pltpu.HBM)


def solution(mesh):
    groups = mesh.shape["dp"]

    def local_step(grad_row, param_blk, accum_blk, learn_rate, clip_max):
        n = grad_row.shape[1] // LANES
        blk = n // groups
        third = -(-blk // 24) * 8
        pad = -(-blk // 8) * 8
        f32 = jnp.float32
        vm = pl.BlockSpec(memory_space=pltpu.VMEM)
        sm = pl.BlockSpec(memory_space=pltpu.SMEM)
        hb = pl.BlockSpec(memory_space=pltpu.HBM)
        dma = pltpu.SemaphoreType.DMA
        full, newa, norm = pl.pallas_call(
            functools.partial(kernel, blk, third, groups),
            out_shape=(
                pltpu.VMEM((n, LANES), f32),
                pltpu.VMEM((blk, LANES), f32),
                pltpu.VMEM((1, LANES), f32),
            ),
            in_specs=[sm, sm, hb, hb, hb],
            out_specs=(vm, vm, vm),
            scratch_shapes=[
                pltpu.VMEM((8, pad, LANES), f32),
                pltpu.VMEM((8, pad, LANES), f32),
                pltpu.VMEM((21, third, LANES), f32),
                pltpu.VMEM((3, FIRST, LANES), f32),
                pltpu.VMEM((3, FIRST, LANES), f32),
                pltpu.VMEM((blk, LANES), f32),
                pltpu.VMEM((blk, LANES), f32),
                pltpu.VMEM((groups, LANES), f32),
                pltpu.VMEM((9, EARLY, LANES), f32),
                dma((3,)), dma((PIECES + 3,)), dma((8,)), dma, dma, dma,
            ],
            compiler_params=pltpu.CompilerParams(
                collective_id=0, has_side_effects=True, vmem_limit_bytes=40 * 1024 * 1024),
        )(learn_rate, clip_max, in_hbm(grad_row.reshape(n, LANES)),
          in_hbm(param_blk.reshape(blk, LANES)), in_hbm(accum_blk.reshape(blk, LANES)))
        newp, newa, copy, norm = pl.pallas_call(
            functools.partial(write_kernel, blk),
            out_shape=(
                jax.ShapeDtypeStruct((blk, LANES), f32),
                jax.ShapeDtypeStruct((blk, LANES), f32),
                jax.ShapeDtypeStruct((n, LANES), jnp.bfloat16),
                jax.ShapeDtypeStruct((1, 1), f32),
            ),
            in_specs=[vm, vm, vm],
            out_specs=(hb, hb, hb, hb),
            scratch_shapes=[pltpu.VMEM((n, LANES), jnp.bfloat16), pltpu.VMEM((1, 1), f32), dma((4,))],
            compiler_params=pltpu.CompilerParams(vmem_limit_bytes=12 * 1024 * 1024),
        )(full, newa, norm)
        return newp.reshape(-1), newa.reshape(-1), copy.reshape(-1), norm.reshape(())

    return jax.shard_map(local_step, mesh=mesh, in_specs=(P("dp", None), P("dp"), P("dp"), P(), P()), out_specs=(P("dp"), P("dp"), P(), P()), check_vma=False)
```

```python
import functools
import jax
import jax.numpy as jnp
from jax import lax
from jax.sharding import PartitionSpec as P
from jax.experimental import pallas as pl
from jax.experimental.pallas import tpu as pltpu

EPS = 1e-10
LANES = 128
X, Y, Z = 1, 2, 4
ORDERS = ((X, Y, Z), (Y, Z, X), (Z, X, Y))
MESH = pl.DeviceIdType.MESH
TILES = 20
PIECES = 6
AHEAD = 106
EARLY = 160
BOTH = 112
FIRST = 64


def cut(start, size, n):
    step = -(-size // (8 * n)) * 8
    return [(start + i * step, min(step, size - i * step)) for i in range(n)]


def kernel(
    blk, third, groups,
    rate_ref, clip_ref, grad_hbm, par_hbm, acc_hbm,
    full, newa_ref, norm_ref,
    own, part, recv, guest, other, par, acc, slots, raw,
    load_sem, near_sem, far_sem, nrm_sem, raw_sem, send_sem,
):
    me = lax.axis_index("dp")
    core = me % 2
    chip = me // 2
    x, y, z = chip % 2, (chip // 2) % 2, chip // 4
    partner = me + 1 - 2 * core
    across = {X: me + 2 - 4 * x, Y: me + 4 - 8 * y, Z: me + 8 - 16 * z}

    def place(m, c):
        xc = 1 - x if m & X else x
        yc = 1 - y if m & Y else y
        zc = 1 - z if m & Z else z
        return 2 * (4 * zc + 2 * yc + xc) + c

    def base(m, c):
        return blk * place(m, c)

    thirds = [(third * t, min(third, blk - third * t)) for t in range(3)]

    def send(src, dst, rcv, dev):
        pltpu.make_async_remote_copy(
            src_ref=src, dst_ref=dst, send_sem=send_sem, recv_sem=rcv,
            device_id=(dev,), device_id_type=MESH).start()

    def wait_rows(sem, n):
        ref = full.at[pl.ds(0, n)]
        pltpu.make_async_copy(ref, ref, sem).wait()

    barrier = pltpu.get_barrier_semaphore()
    near = (across[X], across[Y], across[Z], partner)
    for dev in near:
        pl.semaphore_signal(barrier, inc=1, device_id=(dev,), device_id_type=MESH)

    waves = ((X + Y + Z,), (X + Y, Y + Z, Z + X), (X, Y, Z, 0))
    for i, wave in enumerate(waves):
        for m in wave:
            pltpu.make_async_copy(
                grad_hbm.at[pl.ds(base(m, core), blk)], own.at[m, pl.ds(0, blk)], load_sem.at[i]).start()
    pltpu.make_async_copy(par_hbm, par, load_sem.at[2]).start()
    pltpu.make_async_copy(acc_hbm, acc, load_sem.at[2]).start()

    pl.semaphore_wait(barrier, len(near))

    all_bits = X + Y + Z
    pieces = [cut(s0 + FIRST, size - FIRST, PIECES) for s0, size in thirds]

    def exchange(m, start, size, i):
        send(grad_hbm.at[pl.ds(base(m, 1 - core) + start, size)],
             part.at[m, pl.ds(start, size)], near_sem.at[i], partner)

    for t in range(3):
        s0, _ = thirds[t]
        for c, dst, i in ((core, recv, 0), (1 - core, guest, 7)):
            send(grad_hbm.at[pl.ds(base(all_bits, c) + s0, FIRST)], dst.at[t, pl.ds(0, FIRST)],
                 far_sem.at[i], across[ORDERS[t][0]])
    for p in range(PIECES):
        for t in range(3):
            exchange(all_bits, *pieces[t][p], p)
    for i in (1, 2):
        for m in waves[i]:
            exchange(m, 0, blk, PIECES - 1 + i)

    def fold(m, start, size):
        r = pl.ds(start, size)
        own[m, r] = own[m, r] + part[m, r]

    def unit(step, t):
        a, b, c = ORDERS[t]
        return (b + c, b, c, 0, c, 0, 0)[step]

    PHASE = (0, 0, 0, 0, 1, 1, 2)

    def push(step, t, start, size):
        dim = ORDERS[t][PHASE[step]]
        s0 = thirds[t][0]
        send(own.at[unit(step, t) ^ dim, pl.ds(start, size)],
             recv.at[3 * step + t, pl.ds(start - s0, size)], far_sem.at[step], across[dim])

    load_waits = [len(w) * blk for w in waves]
    wait_rows(load_sem.at[0], load_waits[0])
    for p in range(PIECES):
        wait_rows(near_sem.at[p], sum(pieces[t][p][1] for t in range(3)))
        for t in range(3):
            fold(all_bits, *pieces[t][p])
            push(0, t, *pieces[t][p])
    wait_rows(load_sem.at[1], load_waits[1])
    wait_rows(near_sem.at[PIECES], load_waits[1])
    for step in (1, 2):
        for t in range(3):
            fold(unit(step, t) ^ ORDERS[t][0], *thirds[t])
            push(step, t, *thirds[t])
    wait_rows(load_sem.at[2], load_waits[2] + 2 * blk)
    wait_rows(near_sem.at[PIECES + 1], load_waits[2])
    for t in range(3):
        fold(unit(3, t) ^ ORDERS[t][0], *thirds[t])
        push(3, t, *thirds[t])
    wait_rows(far_sem.at[7], 3 * FIRST)
    send(guest, other, near_sem.at[PIECES + 2], partner)
    for step in range(4):
        for t in range(3):
            fold(unit(step, t), *thirds[t])

    def early(k, src, lo, hi):
        for t in range(3):
            send(src.at[pl.ds(thirds[t][0] + lo, hi - lo)], raw.at[3 * t + k, pl.ds(lo, hi - lo)],
                 raw_sem, across[ORDERS[t][2]])

    total = jnp.zeros((1, LANES), jnp.float32)
    for step in range(7):
        wait_rows(far_sem.at[step], blk)
        if step == 0:
            wait_rows(near_sem.at[PIECES + 2], 3 * FIRST)
        for t in range(3):
            m = unit(step, t)
            s0, size = thirds[t]
            if step == 0:
                r = pl.ds(0, FIRST)
                recv[t, r] = recv[t, r] + other[t, r]
            got = own[m, pl.ds(s0, size)] + recv[3 * step + t, pl.ds(0, size)]
            own[m, pl.ds(s0, size)] = got
            if step in (0, 1):
                push(4 + step, t, *thirds[t])
            if step == 4:
                push(6, t, *thirds[t])
            if step == 6:
                g = got * (1.0 / groups)
                total = total + jnp.sum(g * g, axis=0, keepdims=True)
        if step == 4:
            early(0, par, 0, AHEAD)
            early(1, acc, 0, AHEAD)

    slots[pl.ds(me, 1)] = total
    mine = slots.at[pl.ds(me, 1)]
    for m in (7, 3, 6, 5, 1, 2, 4):
        for c in (1 - core, core):
            send(mine, mine, nrm_sem, place(m, c))
    send(mine, mine, nrm_sem, partner)
    early(2, own.at[0], 0, EARLY)
    early(0, par, AHEAD, EARLY)
    early(1, acc, AHEAD, EARLY)
    wait_rows(nrm_sem, groups - 1)
    square = jnp.sum(jnp.sum(slots[...], axis=0, keepdims=True), axis=1, keepdims=True)
    norm = jnp.sqrt(square)
    norm_ref[...] = jnp.broadcast_to(norm, (1, LANES))
    scale = jnp.minimum(1.0, clip_ref[...] / norm)
    rate = rate_ref[...]

    def rows(m, start, size, c=core):
        return full.at[pl.ds(base(m, c) + start, size)]

    def gather(m, t, j, rcv, start, size):
        send(rows(m, start, size), rows(m, start, size), rcv, across[ORDERS[t][2 - j]])

    def forward(m, start, size, c=core):
        send(rows(m, start, size, c), rows(m, start, size, c), near_sem.at[PIECES], partner)

    def update(w, a, total):
        h = total * (1.0 / groups) * scale
        a_new = a + h * h
        return a_new, w - rate * h / (jnp.sqrt(a_new) + EPS)

    heads = [cut(s0 + EARLY, size - EARLY, 4) + [(s0, EARLY)] for s0, size in thirds]
    for p in range(5):
        for t in range(3):
            start, size = heads[t][p]
            r = pl.ds(start, size)
            newa_ref[r], full[pl.ds(base(0, core) + start, size)] = update(par[r], acc[r], own[0, r])
            if p < 4:
                gather(0, t, 0, far_sem.at[0], start, size)
    for j in (1, 2):
        for t in range(3):
            gather(0, t, j, far_sem.at[j], *thirds[t])
    forward(0, 0, blk)
    wait_rows(raw_sem, 9 * EARLY)
    for t in range(3):
        r = pl.ds(0, EARLY)
        full[pl.ds(base(ORDERS[t][2], core) + thirds[t][0], EARLY)] = update(
            raw[3 * t, r], raw[3 * t + 1, r], raw[3 * t + 2, r])[1]

    tails = [cut(s0, size - BOTH, PIECES) for s0, size in thirds]
    ends = [(s0 + size - BOTH, BOTH) for s0, size in thirds]
    for step in range(6):
        wait_rows(far_sem.at[step], blk if step else blk - 3 * EARLY)
        for t in range(3):
            c, b, a = ORDERS[t]
            m = (a, b, c, a + b, a + c, b + c)[step]
            if step == 0:
                gather(m, t, 1, far_sem.at[3], *thirds[t])
            if step in (0, 1):
                gather(m, t, 2, far_sem.at[4 + step], *thirds[t])
            if step == 3:
                for p in range(PIECES):
                    r = rows(m, *tails[t][p])
                    send(r, r, near_sem.at[p], place(ORDERS[t][0], 1 - core))
        if step == 3:
            last = [(rows(a + b, *ends[t]), c) for t, (c, b, a) in enumerate(ORDERS)]

            @pl.when(core == 0)
            def _():
                for r, c in last:
                    send(r, r, nrm_sem, place(c, 0))

            for r, c in last:
                send(r, r, near_sem.at[PIECES + 1], place(c, 1 - core))
        for t in range(3):
            c, b, a = ORDERS[t]
            forward((a, b, c, a + b, a + c, b + c)[step], *thirds[t])
    for p in range(PIECES):
        wait_rows(near_sem.at[p], sum(tails[t][p][1] for t in range(3)))
        for t in range(3):
            forward(all_bits, *tails[t][p], 1 - core)
    n_both = sum(size for _, size in ends)
    wait_rows(near_sem.at[PIECES + 1], n_both)

    @pl.when(core == 0)
    def _():
        for t in range(3):
            forward(all_bits, *ends[t], 1)
        wait_rows(nrm_sem, n_both)
        wait_rows(near_sem.at[PIECES], 8 * blk - n_both)
        wait_rows(send_sem, 2 * n_both)

    @pl.when(core == 1)
    def _():
        wait_rows(near_sem.at[PIECES], 8 * blk)

    for n in (8 * blk, 7 * blk + 3 * FIRST, groups - 1, 7 * blk - 3 * EARLY, 8 * blk - n_both, 9 * EARLY):
        wait_rows(send_sem, n)


def write_kernel(blk, full, newa, norm, newp_hbm, newa_hbm, copy_hbm, norm_hbm, buf, one, sems):
    me = lax.axis_index("dp")
    mine = full.at[pl.ds(me * blk, blk)]
    one[...] = norm[:, :1]
    out = [
        pltpu.make_async_copy(mine, newp_hbm, sems.at[0]),
        pltpu.make_async_copy(newa, newa_hbm, sems.at[1]),
        pltpu.make_async_copy(one, norm_hbm, sems.at[2]),
    ]
    for cp in out:
        cp.start()
    n = full.shape[0]
    edges = [n * i // TILES // 16 * 16 for i in range(TILES)] + [n]
    for i in range(TILES):
        r = pl.ds(edges[i], edges[i + 1] - edges[i])
        buf[r] = full[r].astype(jnp.bfloat16)
        pltpu.make_async_copy(buf.at[r], copy_hbm.at[r], sems.at[3]).start()
    pltpu.make_async_copy(buf, copy_hbm, sems.at[3]).wait()
    for cp in out:
        cp.wait()


def in_hbm(a):
    return pltpu.with_memory_space_constraint(a, pltpu.HBM)


def solution(mesh):
    groups = mesh.shape["dp"]

    def local_step(grad_row, param_blk, accum_blk, learn_rate, clip_max):
        n = grad_row.shape[1] // LANES
        blk = n // groups
        third = -(-blk // 24) * 8
        pad = -(-blk // 8) * 8
        f32 = jnp.float32
        vm = pl.BlockSpec(memory_space=pltpu.VMEM)
        sm = pl.BlockSpec(memory_space=pltpu.SMEM)
        hb = pl.BlockSpec(memory_space=pltpu.HBM)
        dma = pltpu.SemaphoreType.DMA
        full, newa, norm = pl.pallas_call(
            functools.partial(kernel, blk, third, groups),
            out_shape=(
                pltpu.VMEM((n, LANES), f32),
                pltpu.VMEM((blk, LANES), f32),
                pltpu.VMEM((1, LANES), f32),
            ),
            in_specs=[sm, sm, hb, hb, hb],
            out_specs=(vm, vm, vm),
            scratch_shapes=[
                pltpu.VMEM((8, pad, LANES), f32),
                pltpu.VMEM((8, pad, LANES), f32),
                pltpu.VMEM((21, third, LANES), f32),
                pltpu.VMEM((3, FIRST, LANES), f32),
                pltpu.VMEM((3, FIRST, LANES), f32),
                pltpu.VMEM((blk, LANES), f32),
                pltpu.VMEM((blk, LANES), f32),
                pltpu.VMEM((groups, LANES), f32),
                pltpu.VMEM((9, EARLY, LANES), f32),
                dma((3,)), dma((PIECES + 3,)), dma((8,)), dma, dma, dma,
            ],
            compiler_params=pltpu.CompilerParams(
                collective_id=0, has_side_effects=True, vmem_limit_bytes=40 * 1024 * 1024),
        )(learn_rate, clip_max, in_hbm(grad_row.reshape(n, LANES)),
          in_hbm(param_blk.reshape(blk, LANES)), in_hbm(accum_blk.reshape(blk, LANES)))
        newp, newa, copy, norm = pl.pallas_call(
            functools.partial(write_kernel, blk),
            out_shape=(
                jax.ShapeDtypeStruct((blk, LANES), f32),
                jax.ShapeDtypeStruct((blk, LANES), f32),
                jax.ShapeDtypeStruct((n, LANES), jnp.bfloat16),
                jax.ShapeDtypeStruct((1, 1), f32),
            ),
            in_specs=[vm, vm, vm],
            out_specs=(hb, hb, hb, hb),
            scratch_shapes=[pltpu.VMEM((n, LANES), jnp.bfloat16), pltpu.VMEM((1, 1), f32), dma((4,))],
            compiler_params=pltpu.CompilerParams(vmem_limit_bytes=12 * 1024 * 1024),
        )(full, newa, norm)
        return newp.reshape(-1), newa.reshape(-1), copy.reshape(-1), norm.reshape(())

    return jax.shard_map(local_step, mesh=mesh, in_specs=(P("dp", None), P("dp"), P("dp"), P(), P()), out_specs=(P("dp"), P("dp"), P(), P()), check_vma=False)
```

```python
import functools
import jax
import jax.numpy as jnp
from jax import lax
from jax.sharding import PartitionSpec as P
from jax.experimental import pallas as pl
from jax.experimental.pallas import tpu as pltpu

EPS = 1e-10
LANES = 128
X, Y, Z = 1, 2, 4
ORDERS = ((X, Y, Z), (Y, Z, X), (Z, X, Y))
MESH = pl.DeviceIdType.MESH
TILES = 20
PIECES = 6
AHEAD = 104
EARLY = 160
BOTH = 112
FIRST = 64


def cut(start, size, n):
    step = -(-size // (8 * n)) * 8
    return [(start + i * step, min(step, size - i * step)) for i in range(n)]


def kernel(
    blk, third, groups,
    rate_ref, clip_ref, grad_hbm, par_hbm, acc_hbm,
    full, newa_ref, norm_ref,
    own, part, recv, guest, other, par, acc, slots, raw,
    load_sem, near_sem, far_sem, nrm_sem, raw_sem, send_sem,
):
    me = lax.axis_index("dp")
    core = me % 2
    chip = me // 2
    x, y, z = chip % 2, (chip // 2) % 2, chip // 4
    partner = me + 1 - 2 * core
    across = {X: me + 2 - 4 * x, Y: me + 4 - 8 * y, Z: me + 8 - 16 * z}

    def place(m, c):
        xc = 1 - x if m & X else x
        yc = 1 - y if m & Y else y
        zc = 1 - z if m & Z else z
        return 2 * (4 * zc + 2 * yc + xc) + c

    def base(m, c):
        return blk * place(m, c)

    thirds = [(third * t, min(third, blk - third * t)) for t in range(3)]

    def send(src, dst, rcv, dev):
        pltpu.make_async_remote_copy(
            src_ref=src, dst_ref=dst, send_sem=send_sem, recv_sem=rcv,
            device_id=(dev,), device_id_type=MESH).start()

    def wait_rows(sem, n):
        ref = full.at[pl.ds(0, n)]
        pltpu.make_async_copy(ref, ref, sem).wait()

    barrier = pltpu.get_barrier_semaphore()
    near = (across[X], across[Y], across[Z], partner)
    for dev in near:
        pl.semaphore_signal(barrier, inc=1, device_id=(dev,), device_id_type=MESH)

    waves = ((X + Y + Z,), (X + Y, Y + Z, Z + X), (X, Y, Z, 0))
    for i, wave in enumerate(waves):
        for m in wave:
            pltpu.make_async_copy(
                grad_hbm.at[pl.ds(base(m, core), blk)], own.at[m, pl.ds(0, blk)], load_sem.at[i]).start()
    pltpu.make_async_copy(par_hbm, par, load_sem.at[2]).start()
    pltpu.make_async_copy(acc_hbm, acc, load_sem.at[2]).start()

    pl.semaphore_wait(barrier, len(near))

    all_bits = X + Y + Z
    pieces = [cut(s0 + FIRST, size - FIRST, PIECES) for s0, size in thirds]

    def exchange(m, start, size, i):
        send(grad_hbm.at[pl.ds(base(m, 1 - core) + start, size)],
             part.at[m, pl.ds(start, size)], near_sem.at[i], partner)

    for t in range(3):
        s0, _ = thirds[t]
        for c, dst, i in ((core, recv, 0), (1 - core, guest, 7)):
            send(grad_hbm.at[pl.ds(base(all_bits, c) + s0, FIRST)], dst.at[t, pl.ds(0, FIRST)],
                 far_sem.at[i], across[ORDERS[t][0]])
    for p in range(PIECES):
        for t in range(3):
            exchange(all_bits, *pieces[t][p], p)
    for i in (1, 2):
        for m in waves[i]:
            exchange(m, 0, blk, PIECES - 1 + i)

    def fold(m, start, size):
        r = pl.ds(start, size)
        own[m, r] = own[m, r] + part[m, r]

    def unit(step, t):
        a, b, c = ORDERS[t]
        return (b + c, b, c, 0, c, 0, 0)[step]

    PHASE = (0, 0, 0, 0, 1, 1, 2)

    def push(step, t, start, size):
        dim = ORDERS[t][PHASE[step]]
        s0 = thirds[t][0]
        send(own.at[unit(step, t) ^ dim, pl.ds(start, size)],
             recv.at[3 * step + t, pl.ds(start - s0, size)], far_sem.at[step], across[dim])

    load_waits = [len(w) * blk for w in waves]
    wait_rows(load_sem.at[0], load_waits[0])
    for p in range(PIECES):
        wait_rows(near_sem.at[p], sum(pieces[t][p][1] for t in range(3)))
        for t in range(3):
            fold(all_bits, *pieces[t][p])
            push(0, t, *pieces[t][p])
    wait_rows(load_sem.at[1], load_waits[1])
    wait_rows(near_sem.at[PIECES], load_waits[1])
    for step in (1, 2):
        for t in range(3):
            fold(unit(step, t) ^ ORDERS[t][0], *thirds[t])
            push(step, t, *thirds[t])
    wait_rows(load_sem.at[2], load_waits[2] + 2 * blk)
    wait_rows(near_sem.at[PIECES + 1], load_waits[2])
    for t in range(3):
        fold(unit(3, t) ^ ORDERS[t][0], *thirds[t])
        push(3, t, *thirds[t])
    wait_rows(far_sem.at[7], 3 * FIRST)
    send(guest, other, near_sem.at[PIECES + 2], partner)
    for step in range(4):
        for t in range(3):
            fold(unit(step, t), *thirds[t])

    def early(k, src, lo, hi):
        for t in range(3):
            send(src.at[pl.ds(thirds[t][0] + lo, hi - lo)], raw.at[3 * t + k, pl.ds(lo, hi - lo)],
                 raw_sem, across[ORDERS[t][2]])

    total = jnp.zeros((1, LANES), jnp.float32)
    for step in range(7):
        wait_rows(far_sem.at[step], blk)
        if step == 0:
            wait_rows(near_sem.at[PIECES + 2], 3 * FIRST)
        for t in range(3):
            m = unit(step, t)
            s0, size = thirds[t]
            if step == 0:
                r = pl.ds(0, FIRST)
                recv[t, r] = recv[t, r] + other[t, r]
            got = own[m, pl.ds(s0, size)] + recv[3 * step + t, pl.ds(0, size)]
            own[m, pl.ds(s0, size)] = got
            if step in (0, 1):
                push(4 + step, t, *thirds[t])
            if step == 4:
                push(6, t, *thirds[t])
            if step == 6:
                g = got * (1.0 / groups)
                total = total + jnp.sum(g * g, axis=0, keepdims=True)
        if step == 4:
            early(0, par, 0, AHEAD)
            early(1, acc, 0, AHEAD)

    slots[pl.ds(me, 1)] = total
    mine = slots.at[pl.ds(me, 1)]
    for m in (7, 3, 6, 5, 1, 2, 4):
        for c in (1 - core, core):
            send(mine, mine, nrm_sem, place(m, c))
    send(mine, mine, nrm_sem, partner)
    early(2, own.at[0], 0, EARLY)
    early(0, par, AHEAD, EARLY)
    early(1, acc, AHEAD, EARLY)
    wait_rows(nrm_sem, groups - 1)
    square = jnp.sum(jnp.sum(slots[...], axis=0, keepdims=True), axis=1, keepdims=True)
    norm = jnp.sqrt(square)
    norm_ref[...] = jnp.broadcast_to(norm, (1, LANES))
    scale = jnp.minimum(1.0, clip_ref[...] / norm)
    rate = rate_ref[...]

    def rows(m, start, size, c=core):
        return full.at[pl.ds(base(m, c) + start, size)]

    def gather(m, t, j, rcv, start, size):
        send(rows(m, start, size), rows(m, start, size), rcv, across[ORDERS[t][2 - j]])

    def forward(m, start, size, c=core):
        send(rows(m, start, size, c), rows(m, start, size, c), near_sem.at[PIECES], partner)

    def update(w, a, total):
        h = total * (1.0 / groups) * scale
        a_new = a + h * h
        return a_new, w - rate * h / (jnp.sqrt(a_new) + EPS)

    heads = [cut(s0 + EARLY, size - EARLY, 4) + [(s0, EARLY)] for s0, size in thirds]
    for p in range(5):
        for t in range(3):
            start, size = heads[t][p]
            r = pl.ds(start, size)
            newa_ref[r], full[pl.ds(base(0, core) + start, size)] = update(par[r], acc[r], own[0, r])
            if p < 4:
                gather(0, t, 0, far_sem.at[0], start, size)
    for j in (1, 2):
        for t in range(3):
            gather(0, t, j, far_sem.at[j], *thirds[t])
    forward(0, 0, blk)
    wait_rows(raw_sem, 9 * EARLY)
    for t in range(3):
        r = pl.ds(0, EARLY)
        full[pl.ds(base(ORDERS[t][2], core) + thirds[t][0], EARLY)] = update(
            raw[3 * t, r], raw[3 * t + 1, r], raw[3 * t + 2, r])[1]

    tails = [cut(s0, size - BOTH, PIECES) for s0, size in thirds]
    ends = [(s0 + size - BOTH, BOTH) for s0, size in thirds]
    for step in range(6):
        wait_rows(far_sem.at[step], blk if step else blk - 3 * EARLY)
        for t in range(3):
            c, b, a = ORDERS[t]
            m = (a, b, c, a + b, a + c, b + c)[step]
            if step == 0:
                gather(m, t, 1, far_sem.at[3], *thirds[t])
            if step in (0, 1):
                gather(m, t, 2, far_sem.at[4 + step], *thirds[t])
            if step == 3:
                for p in range(PIECES):
                    r = rows(m, *tails[t][p])
                    send(r, r, near_sem.at[p], place(ORDERS[t][0], 1 - core))
        if step == 3:
            last = [(rows(a + b, *ends[t]), c) for t, (c, b, a) in enumerate(ORDERS)]

            @pl.when(core == 0)
            def _():
                for r, c in last:
                    send(r, r, nrm_sem, place(c, 0))

            for r, c in last:
                send(r, r, near_sem.at[PIECES + 1], place(c, 1 - core))
        for t in range(3):
            c, b, a = ORDERS[t]
            forward((a, b, c, a + b, a + c, b + c)[step], *thirds[t])
    for p in range(PIECES):
        wait_rows(near_sem.at[p], sum(tails[t][p][1] for t in range(3)))
        for t in range(3):
            forward(all_bits, *tails[t][p], 1 - core)
    n_both = sum(size for _, size in ends)
    wait_rows(near_sem.at[PIECES + 1], n_both)

    @pl.when(core == 0)
    def _():
        for t in range(3):
            forward(all_bits, *ends[t], 1)
        wait_rows(nrm_sem, n_both)
        wait_rows(near_sem.at[PIECES], 8 * blk - n_both)
        wait_rows(send_sem, 2 * n_both)

    @pl.when(core == 1)
    def _():
        wait_rows(near_sem.at[PIECES], 8 * blk)

    for n in (8 * blk, 7 * blk + 3 * FIRST, groups - 1, 7 * blk - 3 * EARLY, 8 * blk - n_both, 9 * EARLY):
        wait_rows(send_sem, n)


def write_kernel(blk, full, newa, norm, newp_hbm, newa_hbm, copy_hbm, norm_hbm, buf, one, sems):
    me = lax.axis_index("dp")
    mine = full.at[pl.ds(me * blk, blk)]
    one[...] = norm[:, :1]
    out = [
        pltpu.make_async_copy(mine, newp_hbm, sems.at[0]),
        pltpu.make_async_copy(newa, newa_hbm, sems.at[1]),
        pltpu.make_async_copy(one, norm_hbm, sems.at[2]),
    ]
    for cp in out:
        cp.start()
    n = full.shape[0]
    edges = [n * i // TILES // 16 * 16 for i in range(TILES)] + [n]
    for i in range(TILES):
        r = pl.ds(edges[i], edges[i + 1] - edges[i])
        buf[r] = full[r].astype(jnp.bfloat16)
        pltpu.make_async_copy(buf.at[r], copy_hbm.at[r], sems.at[3]).start()
    pltpu.make_async_copy(buf, copy_hbm, sems.at[3]).wait()
    for cp in out:
        cp.wait()


def in_hbm(a):
    return pltpu.with_memory_space_constraint(a, pltpu.HBM)


def solution(mesh):
    groups = mesh.shape["dp"]

    def local_step(grad_row, param_blk, accum_blk, learn_rate, clip_max):
        n = grad_row.shape[1] // LANES
        blk = n // groups
        third = -(-blk // 24) * 8
        pad = -(-blk // 8) * 8
        f32 = jnp.float32
        vm = pl.BlockSpec(memory_space=pltpu.VMEM)
        sm = pl.BlockSpec(memory_space=pltpu.SMEM)
        hb = pl.BlockSpec(memory_space=pltpu.HBM)
        dma = pltpu.SemaphoreType.DMA
        full, newa, norm = pl.pallas_call(
            functools.partial(kernel, blk, third, groups),
            out_shape=(
                pltpu.VMEM((n, LANES), f32),
                pltpu.VMEM((blk, LANES), f32),
                pltpu.VMEM((1, LANES), f32),
            ),
            in_specs=[sm, sm, hb, hb, hb],
            out_specs=(vm, vm, vm),
            scratch_shapes=[
                pltpu.VMEM((8, pad, LANES), f32),
                pltpu.VMEM((8, pad, LANES), f32),
                pltpu.VMEM((21, third, LANES), f32),
                pltpu.VMEM((3, FIRST, LANES), f32),
                pltpu.VMEM((3, FIRST, LANES), f32),
                pltpu.VMEM((blk, LANES), f32),
                pltpu.VMEM((blk, LANES), f32),
                pltpu.VMEM((groups, LANES), f32),
                pltpu.VMEM((9, EARLY, LANES), f32),
                dma((3,)), dma((PIECES + 3,)), dma((8,)), dma, dma, dma,
            ],
            compiler_params=pltpu.CompilerParams(
                collective_id=0, has_side_effects=True, vmem_limit_bytes=40 * 1024 * 1024),
        )(learn_rate, clip_max, in_hbm(grad_row.reshape(n, LANES)),
          in_hbm(param_blk.reshape(blk, LANES)), in_hbm(accum_blk.reshape(blk, LANES)))
        newp, newa, copy, norm = pl.pallas_call(
            functools.partial(write_kernel, blk),
            out_shape=(
                jax.ShapeDtypeStruct((blk, LANES), f32),
                jax.ShapeDtypeStruct((blk, LANES), f32),
                jax.ShapeDtypeStruct((n, LANES), jnp.bfloat16),
                jax.ShapeDtypeStruct((1, 1), f32),
            ),
            in_specs=[vm, vm, vm],
            out_specs=(hb, hb, hb, hb),
            scratch_shapes=[pltpu.VMEM((n, LANES), jnp.bfloat16), pltpu.VMEM((1, 1), f32), dma((4,))],
            compiler_params=pltpu.CompilerParams(vmem_limit_bytes=12 * 1024 * 1024),
        )(full, newa, norm)
        return newp.reshape(-1), newa.reshape(-1), copy.reshape(-1), norm.reshape(())

    return jax.shard_map(local_step, mesh=mesh, in_specs=(P("dp", None), P("dp"), P("dp"), P(), P()), out_specs=(P("dp"), P("dp"), P(), P()), check_vma=False)
```
